16 devices in a mesh: dp: 1, tp: 16 (over x, y, z, core).
Axes of the slice: x: 2, y: 2, z: 2, core: 2. Of those that a mesh axis runs over, the one named last changes fastest.
Arguments:
- x: bfloat16 [2048, 5120], P('dp')
- dy: bfloat16 [2048, 5120], P('dp')
- gate: bfloat16 [2048, 12288], P('dp', 'tp')
- up: bfloat16 [2048, 12288], P('dp', 'tp')
- w_gate: bfloat16 [5120, 12288], P(None, 'tp')
- w_up: bfloat16 [5120, 12288], P(None, 'tp')
- w_down: bfloat16 [12288, 5120], P('tp')
Outputs:
- output 1: bfloat16 [2048, 5120], P('dp')
- output 2: bfloat16 [5120, 12288], P('dp', 'tp')
- output 3: bfloat16 [5120, 12288], P('dp', 'tp')
- output 4: bfloat16 [12288, 5120], P(('dp', 'tp'))
All inputs are finite; a program needn't handle non-finite values.
Results may differ from the reference program's by a relative error of at most 0.012.
Values are sent between devices in bfloat16 or wider.
A program may use at most 2 GiB of HBM per device.

```python
import jax
import jax.numpy as jnp

ROWS = 2048
D = 5120
FF = 12288


def act(gate, up):
    return jax.nn.silu(gate) * up


def setup_inputs(seed: int = 0, part: int = 0) -> dict:
    kx, ky, ka, kb, kg, ku, kd = jax.random.split(jax.random.key(seed), 7)
    kx, ky, ka, kb = (jax.random.fold_in(k, part) for k in (kx, ky, ka, kb))
    drawn = {
        "x": jax.random.normal(kx, (ROWS, D), jnp.float32),
        "dy": jax.random.normal(ky, (ROWS, D), jnp.float32),
        "gate": jax.random.normal(ka, (ROWS, FF), jnp.float32),
        "up": jax.random.normal(kb, (ROWS, FF), jnp.float32),
        "w_gate": jax.random.normal(kg, (D, FF), jnp.float32) * D**-0.5,
        "w_up": jax.random.normal(ku, (D, FF), jnp.float32) * D**-0.5,
        "w_down": jax.random.normal(kd, (FF, D), jnp.float32) * FF**-0.5,
    }
    return {k: v.astype(jnp.bfloat16) for k, v in drawn.items()}


def reference(x, dy, gate, up, w_gate, w_up, w_down):
    hidden, back = jax.vjp(act, gate.astype(jnp.float32), up.astype(jnp.float32))
    d_hidden = jnp.dot(dy, w_down.T, preferred_element_type=jnp.float32)
    d_gate, d_up = (g.astype(jnp.bfloat16) for g in back(d_hidden))
    dx = jnp.dot(d_gate, w_gate.T, preferred_element_type=jnp.float32) + jnp.dot(d_up, w_up.T, preferred_element_type=jnp.float32)
    dw_gate = jnp.dot(x.T, d_gate, preferred_element_type=jnp.float32)
    dw_up = jnp.dot(x.T, d_up, preferred_element_type=jnp.float32)
    dw_down = jnp.dot(hidden.astype(jnp.bfloat16).T, dy, preferred_element_type=jnp.float32)
    return tuple(g.astype(jnp.bfloat16) for g in (dx, dw_gate, dw_up, dw_down))
```

```python
import functools

import jax
import jax.numpy as jnp
from jax import lax
from jax.experimental import pallas as pl
from jax.experimental.pallas import tpu as pltpu
from jax.sharding import PartitionSpec as P

MESH = pl.DeviceIdType.MESH
BF, F32 = jnp.bfloat16, jnp.float32
NT = (((1,), (1,)), ((), ()))
TN = (((0,), (0,)), ((), ()))
NN = (((1,), (0,)), ((), ()))
NG = 8
ORDERS = ((8, 4, 2), (4, 2, 8), (2, 8, 4))


def dot(a, b, dims):
    return lax.dot_general(a, b, dims, preferred_element_type=F32)


def colours(half):
    tiles = half // 128
    widths = [128 * ((tiles + 2 - k) // 3) for k in range(3)]
    return [(sum(widths[:k]), widths[k]) for k in range(3)]


def kernel(
    x, dy, gate, up, w_gate, w_up, w_down,
    dx, dw_gate, dw_up, dw_down,
    d_all, hid_t, acc0, acc1, acc2, acc3, d2d_out, d2d_in, out1, out2, out3, in1, in2, in3, fin,
    load, d2d_s, d2d_r, s1, s2, s3, r1, r2, r3, a_loc, a3s, a3r, a2s, a2r, a1s, a1r, ds, dr, credit, st,
    *, cb,
):
    rows, wide = x.shape
    ff = gate.shape[1]
    g_rows, half = rows // NG, wide // 2
    cols = colours(half)
    steps = wide // cb
    me = lax.axis_index("tp")
    core = lax.rem(me, 2)
    sib = me + 1 - 2 * core
    mine = pl.multiple_of(core * half, 128)
    other = pl.multiple_of((1 - core) * half, 128)

    def bit(stride):
        return lax.rem(me // stride, 2)

    def peer(stride):
        return me + (1 - 2 * bit(stride)) * stride

    def rows_at(start, size):
        return pl.ds(pl.multiple_of(start, size), size)

    def remote(src, dst, send, recv, to):
        return pltpu.make_async_remote_copy(
            src_ref=src, dst_ref=dst, send_sem=send, recv_sem=recv,
            device_id={"tp": to}, device_id_type=MESH,
        )

    def c_d2d():
        return remote(d2d_out, d2d_in, d2d_s, d2d_r, sib)

    def c_rs(stage, g, k):
        src, dst, send, recv = ((out1, in1, s1, r1), (out2, in2, s2, r2), (out3, in3, s3, r3))[stage]
        c = pl.ds(*cols[k])
        return remote(src.at[:, c], dst.at[g, :, c], send.at[k], recv.at[k, g], peer(ORDERS[k][stage]))

    def region(g, k, depth):
        start, size = g * g_rows, g_rows
        for stage in range(depth):
            size //= 2
            start = start + bit(ORDERS[k][stage]) * size
        return dx.at[rows_at(start, size), pl.ds(pl.multiple_of(mine + cols[k][0], 128), cols[k][1])]

    def c_local(g, k):
        return pltpu.make_async_copy(fin.at[g, :, pl.ds(*cols[k])], region(g, k, 3), a_loc.at[k, g])

    def c_a0(g, k):
        return remote(fin.at[g, :, pl.ds(*cols[k])], region(g, k, 3), a3s.at[k, g], a3r.at[k, g], peer(ORDERS[k][2]))

    def c_a1(g, k):
        return remote(region(g, k, 2), region(g, k, 2), a2s.at[k, g], a2r.at[k, g], peer(ORDERS[k][1]))

    def c_a2(g, k):
        return remote(region(g, k, 1), region(g, k, 1), a1s.at[k, g], a1r.at[k, g], peer(ORDERS[k][0]))

    def c_a3(g, k):
        return remote(region(g, k, 0), region(g, k, 0), ds.at[k, g], dr.at[k, g], sib)

    def e1(g):
        c_d2d().wait_recv()
        h = g_rows // 2
        for k in range(3):
            c = pl.ds(*cols[k])
            away = rows_at((1 - bit(ORDERS[k][0])) * h, h)

            @pl.when(g > 0)
            def _():
                c_rs(0, g, k).wait_send()

            out1[:, c] = (acc0[away, c] + d2d_in[away, c].astype(F32)).astype(BF)
            c_rs(0, g, k).start()
        for k in range(3):
            c = pl.ds(*cols[k])
            keep = rows_at(bit(ORDERS[k][0]) * h, h)
            acc1[:, c] = acc0[keep, c] + d2d_in[keep, c].astype(F32)

        @pl.when(g < NG - 1)
        def _():
            pl.semaphore_signal(credit, inc=1, device_id={"tp": sib}, device_id_type=MESH)

    def e_mid(stage, g, src, came, out, dst):
        h = src.shape[0] // 2
        for k in range(3):
            c = pl.ds(*cols[k])
            c_rs(stage - 1, g, k).wait_recv()
            away = rows_at((1 - bit(ORDERS[k][stage])) * h, h)

            @pl.when(g > 0)
            def _():
                c_rs(stage, g, k).wait_send()

            out[:, c] = (src[away, c] + came[g, away, c].astype(F32)).astype(BF)
            c_rs(stage, g, k).start()
            keep = rows_at(bit(ORDERS[k][stage]) * h, h)
            dst[:, c] = src[keep, c] + came[g, keep, c].astype(F32)

    def e4(g):
        for k in range(3):
            c = pl.ds(*cols[k])
            c_rs(2, g, k).wait_recv()
            fin[g, :, c] = (acc3[:, c] + in3[g, :, c].astype(F32)).astype(BF)
            c_local(g, k).start()

    def a0(g):
        for k in range(3):
            c_a0(g, k).start()

    def at(cond, f, g):
        @pl.when(cond)
        def _():
            f(g)

    def reduce_events(t):
        at((t >= 3) & (t < NG + 3), e4, t - 3)
        at((t >= 2) & (t < NG + 2), lambda g: e_mid(2, g, acc2, in2, out3, acc3), t - 2)
        at((t >= 1) & (t < NG + 1), lambda g: e_mid(1, g, acc1, in1, out2, acc2), t - 1)

    def a1(g):
        for k in range(3):
            c_local(g, k).wait()
            c_a0(g, k).wait_recv()
            c_a1(g, k).start()

    def a2(g):
        for k in range(3):
            c_a1(g, k).wait_recv()
            c_a2(g, k).start()

    def a3(g):
        for k in range(3):
            c_a2(g, k).wait_recv()
            c_a3(g, k).start()

    def slot(s):
        @pl.when(s < 3)
        def _():
            reduce_events(NG + s)
            at(s >= 0, a0, NG + s - 3)

        for lag, f in ((5, a3), (3, a2), (1, a1)):
            t = s - lag
            g = lax.div(2 * jnp.maximum(t, 0), 5)
            at((t >= 0) & (lax.rem(2 * jnp.maximum(t, 0), 5) < 2) & (g < NG), f, g)

    last_slot = 5 + (5 * (NG - 1) + 1) // 2

    barrier = pltpu.get_barrier_semaphore()
    for to in (sib, peer(8), peer(4), peer(2)):
        pl.semaphore_signal(barrier, inc=1, device_id={"tp": to}, device_id_type=MESH)
    pl.semaphore_wait(barrier, 4)

    def first_phase(wd, wg, wu, dyb, gb, ub):
        def rows_of(g):
            r = rows_at(g * g_rows, g_rows)
            return (
                pltpu.make_async_copy(dy.at[r], dyb, load.at[0]),
                pltpu.make_async_copy(gate.at[r], gb, load.at[1]),
                pltpu.make_async_copy(up.at[r], ub, load.at[2]),
            )

        weights = [pltpu.make_async_copy(a, b, load.at[3 + i]) for i, (a, b) in enumerate(((w_down, wd), (w_gate, wg), (w_up, wu)))]
        weights[0].start()
        for c in rows_of(0):
            c.start()
        weights[1].start()
        weights[2].start()
        weights[0].wait()

        def body(g, _):
            for c in rows_of(g):
                c.wait()
            d_h = dot(dyb[...], wd[...], NT)
            gf, uf = gb[...].astype(F32), ub[...].astype(F32)
            sig = jax.nn.sigmoid(gf)
            silu = gf * sig
            r = rows_at(g * g_rows, g_rows)
            d_all[r, pl.ds(0, ff)] = (d_h * uf * (sig + silu * (1 - sig))).astype(BF)
            d_all[r, pl.ds(ff, ff)] = (d_h * silu).astype(BF)
            hid_t[:, r] = (silu * uf).astype(BF).T

            @pl.when(g < NG - 1)
            def _():
                for c in rows_of(jnp.minimum(g + 1, NG - 1)):
                    c.start()

            @pl.when(g == 0)
            def _():
                weights[1].wait()
                weights[2].wait()

            dg, du = d_all[r, pl.ds(0, ff)], d_all[r, pl.ds(ff, ff)]

            def term(start):
                w = pl.ds(start, half)
                return dot(dg, wg[w, :], NT) + dot(du, wu[w, :], NT)

            @pl.when(g > 0)
            def _():
                c_d2d().wait_send()

            d2d_out[...] = term(other).astype(BF)

            @pl.when(g > 0)
            def _():
                pl.semaphore_wait(credit, 1)

            c_d2d().start()
            acc0[...] = term(mine)
            reduce_events(g)
            e1(g)
            return 0

        lax.fori_loop(0, NG, body, 0)

    pl.run_scoped(
        first_phase,
        pltpu.VMEM((ff, wide), BF),
        pltpu.VMEM((wide, ff), BF),
        pltpu.VMEM((wide, ff), BF),
        pltpu.VMEM((g_rows, wide), BF),
        pltpu.VMEM((g_rows, ff), BF),
        pltpu.VMEM((g_rows, ff), BF),
    )

    def second_phase(xb, yb, og, od):
        def loads(i, b):
            c = rows_at(i * cb, cb)
            return (
                pltpu.make_async_copy(x.at[:, c], xb.at[b], load.at[b]),
                pltpu.make_async_copy(dy.at[:, c], yb.at[b], load.at[2 + b]),
            )

        def stores(i, b):
            c = rows_at(i * cb, cb)
            return (
                pltpu.make_async_copy(og.at[b, :, pl.ds(0, ff)], dw_gate.at[c], st.at[b, 0]),
                pltpu.make_async_copy(og.at[b, :, pl.ds(ff, ff)], dw_up.at[c], st.at[b, 1]),
                pltpu.make_async_copy(od.at[b], dw_down.at[:, c], st.at[b, 2]),
            )

        for c in loads(0, 0):
            c.start()

        def early(g, _):
            a0(g)
            return 0

        lax.fori_loop(0, NG - 3, early, 0)

        def body(i, _):
            b = lax.rem(i, 2)

            @pl.when(i < steps - 1)
            def _():
                for c in loads(jnp.minimum(i + 1, steps - 1), 1 - b):
                    c.start()

            into = loads(i, b)
            out = stores(i, b)

            @pl.when(i >= 2)
            def _():
                for c in out:
                    c.wait()

            into[0].wait()
            og[b] = dot(xb[b], d_all[...], TN).astype(BF)
            out[0].start()
            out[1].start()
            slot(2 * i)
            into[1].wait()
            od[b] = dot(hid_t[...], yb[b], NN).astype(BF)
            out[2].start()
            slot(2 * i + 1)
            return 0

        lax.fori_loop(0, steps, body, 0)

        for i in (steps - 2, steps - 1):
            for c in stores(i, i % 2):
                c.wait()

    pl.run_scoped(
        second_phase,
        pltpu.VMEM((2, rows, cb), BF),
        pltpu.VMEM((2, rows, cb), BF),
        pltpu.VMEM((2, cb, 2 * ff), BF),
        pltpu.VMEM((2, ff, cb), BF),
    )

    def rest(s, _):
        slot(s)
        return 0

    lax.fori_loop(2 * steps, last_slot + 1, rest, 0)

    for k in range(3):
        for stage in range(3):
            c_rs(stage, NG - 1, k).wait_send()
    c_d2d().wait_send()

    def drain(g, _):
        for k in range(3):
            c_a0(g, k).wait_send()
            c_a1(g, k).wait_send()
            c_a2(g, k).wait_send()
            c_a3(g, k).wait()
        return 0

    lax.fori_loop(0, NG, drain, 0)


def backward(x, dy, gate, up, w_gate, w_up, w_down, *, cb=512):
    rows, wide = x.shape
    ff = gate.shape[1]
    gr, half = rows // NG, wide // 2
    any_space = pl.BlockSpec(memory_space=pl.ANY)
    dma = pltpu.SemaphoreType.DMA
    return pl.pallas_call(
        functools.partial(kernel, cb=cb),
        out_shape=(
            jax.ShapeDtypeStruct((rows, wide), BF),
            jax.ShapeDtypeStruct((wide, ff), BF),
            jax.ShapeDtypeStruct((wide, ff), BF),
            jax.ShapeDtypeStruct((ff, wide), BF),
        ),
        in_specs=[any_space] * 7,
        out_specs=(any_space,) * 4,
        scratch_shapes=[
            pltpu.VMEM((rows, 2 * ff), BF),
            pltpu.VMEM((ff, rows), BF),
            pltpu.VMEM((gr, half), F32),
            pltpu.VMEM((gr // 2, half), F32),
            pltpu.VMEM((gr // 4, half), F32),
            pltpu.VMEM((gr // 8, half), F32),
            pltpu.VMEM((gr, half), BF),
            pltpu.VMEM((gr, half), BF),
            pltpu.VMEM((gr // 2, half), BF),
            pltpu.VMEM((gr // 4, half), BF),
            pltpu.VMEM((gr // 8, half), BF),
            pltpu.VMEM((NG, gr // 2, half), BF),
            pltpu.VMEM((NG, gr // 4, half), BF),
            pltpu.VMEM((NG, gr // 8, half), BF),
            pltpu.VMEM((NG, gr // 8, half), BF),
            dma((6,)),
            dma(()),
            dma(()),
            dma((3,)),
            dma((3,)),
            dma((3,)),
            *[dma((3, NG))] * 3,
            dma((3, NG)),
            *[dma((3, NG))] * 8,
            pltpu.SemaphoreType.REGULAR,
            dma((2, 3)),
        ],
        compiler_params=pltpu.CompilerParams(
            collective_id=0, has_side_effects=True, vmem_limit_bytes=67_043_328
        ),
        name="mlp_backward",
    )(x, dy, gate, up, w_gate, w_up, w_down)


def solution(mesh):
    tokens, columns, rows = P("dp", None), P(None, "tp"), P("tp", None)
    return jax.shard_map(
        backward,
        mesh=mesh,
        in_specs=(tokens, tokens, P("dp", "tp"), P("dp", "tp"), columns, columns, rows),
        out_specs=(tokens, P("dp", "tp"), P("dp", "tp"), P(("dp", "tp"), None)),
        check_vma=False,
    )
```

```python
import functools

import jax
import jax.numpy as jnp
from jax import lax
from jax.experimental import pallas as pl
from jax.experimental.pallas import tpu as pltpu
from jax.sharding import PartitionSpec as P

MESH = pl.DeviceIdType.MESH
BF, F32 = jnp.bfloat16, jnp.float32
NT = (((1,), (1,)), ((), ()))
TN = (((0,), (0,)), ((), ()))
NN = (((1,), (0,)), ((), ()))
NG = 8
ORDERS = ((8, 4, 2), (4, 2, 8), (2, 8, 4))


def dot(a, b, dims):
    return lax.dot_general(a, b, dims, preferred_element_type=F32)


def colours(half):
    tiles = half // 128
    widths = [128 * ((tiles + 2 - k) // 3) for k in range(3)]
    return [(sum(widths[:k]), widths[k]) for k in range(3)]


def kernel(
    x, dy, gate, up, w_gate, w_up, w_down,
    dx, dw_gate, dw_up, dw_down,
    d_all, hid_t, acc0, acc1, acc2, acc3, d2d_out, d2d_in, out1, out2, out3, in1, in2, in3, fin,
    load, d2d_s, d2d_r, s1, s2, s3, r1, r2, r3, a_loc, a3s, a3r, a2s, a2r, a1s, a1r, ds, dr, credit,
    *, cb,
):
    rows, wide = x.shape
    ff = gate.shape[1]
    g_rows, half = rows // NG, wide // 2
    cols = colours(half)
    steps = wide // cb
    me = lax.axis_index("tp")
    core = lax.rem(me, 2)
    sib = me + 1 - 2 * core
    mine = pl.multiple_of(core * half, 128)
    other = pl.multiple_of((1 - core) * half, 128)

    def stride_of(k, stage):
        first, second = ORDERS[k][stage], ORDERS[(k + 1) % 3][stage]
        return first + core * (second - first)

    def bit(stride):
        return lax.rem(lax.div(me, stride), 2)

    def peer(stride):
        return me + (1 - 2 * bit(stride)) * stride

    def rows_at(start, size):
        return pl.ds(pl.multiple_of(start, size), size)

    def remote(src, dst, send, recv, to):
        return pltpu.make_async_remote_copy(
            src_ref=src, dst_ref=dst, send_sem=send, recv_sem=recv,
            device_id={"tp": to}, device_id_type=MESH,
        )

    def c_d2d():
        return remote(d2d_out, d2d_in, d2d_s, d2d_r, sib)

    def c_rs(stage, g, k):
        src, dst, send, recv = ((out1, in1, s1, r1), (out2, in2, s2, r2), (out3, in3, s3, r3))[stage]
        c = pl.ds(*cols[k])
        return remote(src.at[:, c], dst.at[g, :, c], send.at[k], recv.at[k, g], peer(stride_of(k, stage)))

    def region(g, k, depth):
        start, size = g * g_rows, g_rows
        for stage in range(depth):
            size //= 2
            start = start + bit(stride_of(k, stage)) * size
        return dx.at[rows_at(start, size), pl.ds(pl.multiple_of(mine + cols[k][0], 128), cols[k][1])]

    def c_local(g, k):
        return pltpu.make_async_copy(fin.at[g, :, pl.ds(*cols[k])], region(g, k, 3), a_loc.at[k, g])

    def c_a0(g, k):
        return remote(fin.at[g, :, pl.ds(*cols[k])], region(g, k, 3), a3s.at[k, g], a3r.at[k, g], peer(stride_of(k, 2)))

    def c_a1(g, k):
        return remote(region(g, k, 2), region(g, k, 2), a2s.at[k, g], a2r.at[k, g], peer(stride_of(k, 1)))

    def c_a2(g, k):
        return remote(region(g, k, 1), region(g, k, 1), a1s.at[k, g], a1r.at[k, g], peer(stride_of(k, 0)))

    def c_a3(g, k):
        return remote(region(g, k, 0), region(g, k, 0), ds.at[k, g], dr.at[k, g], sib)

    def e1(g):
        c_d2d().wait_recv()
        h = g_rows // 2
        for k in range(3):
            c = pl.ds(*cols[k])
            away = rows_at((1 - bit(stride_of(k, 0))) * h, h)

            @pl.when(g > 0)
            def _():
                c_rs(0, g, k).wait_send()

            out1[:, c] = (acc0[away, c] + d2d_in[away, c].astype(F32)).astype(BF)
            c_rs(0, g, k).start()
        for k in range(3):
            c = pl.ds(*cols[k])
            keep = rows_at(bit(stride_of(k, 0)) * h, h)
            acc1[:, c] = acc0[keep, c] + d2d_in[keep, c].astype(F32)

        @pl.when(g < NG - 1)
        def _():
            pl.semaphore_signal(credit, inc=1, device_id={"tp": sib}, device_id_type=MESH)

    def e_mid(stage, g, src, came, out, dst):
        h = src.shape[0] // 2
        for k in range(3):
            c = pl.ds(*cols[k])
            c_rs(stage - 1, g, k).wait_recv()
            away = rows_at((1 - bit(stride_of(k, stage))) * h, h)

            @pl.when(g > 0)
            def _():
                c_rs(stage, g, k).wait_send()

            out[:, c] = (src[away, c] + came[g, away, c].astype(F32)).astype(BF)
            c_rs(stage, g, k).start()
            keep = rows_at(bit(stride_of(k, stage)) * h, h)
            dst[:, c] = src[keep, c] + came[g, keep, c].astype(F32)

    def e4(g):
        for k in range(3):
            c = pl.ds(*cols[k])
            c_rs(2, g, k).wait_recv()
            fin[g, :, c] = (acc3[:, c] + in3[g, :, c].astype(F32)).astype(BF)
            c_local(g, k).start()

    def a0(g):
        for k in range(3):
            c_a0(g, k).start()

    def at(cond, f, g):
        @pl.when(cond)
        def _():
            f(g)

    def reduce_events(t):
        at((t >= 3) & (t < NG + 3), e4, t - 3)
        at((t >= 2) & (t < NG + 2), lambda g: e_mid(2, g, acc2, in2, out3, acc3), t - 2)
        at((t >= 1) & (t < NG + 1), lambda g: e_mid(1, g, acc1, in1, out2, acc2), t - 1)

    def a1(g):
        for k in range(3):
            c_local(g, k).wait()
            c_a0(g, k).wait_recv()
            c_a1(g, k).start()

    def a2(g):
        for k in range(3):
            c_a1(g, k).wait_recv()
            c_a2(g, k).start()

    def a3(g):
        for k in range(3):
            c_a2(g, k).wait_recv()
            c_a3(g, k).start()

    def slot(s):
        @pl.when(s < 3)
        def _():
            reduce_events(NG + s)
            at(s >= 0, a0, NG + s - 3)

        for first, num, den, f in ((6, 2, 1, a3), (3, 8, 5, a2), (1, 1, 1, a1)):
            t = den * jnp.maximum(s - first, 0)
            g = lax.div(t, num)
            at((s >= first) & (lax.rem(t, num) < den) & (g < NG), f, g)

    last_slot = 6 + 2 * (NG - 1)

    barrier = pltpu.get_barrier_semaphore()
    for to in (sib, peer(8), peer(4), peer(2)):
        pl.semaphore_signal(barrier, inc=1, device_id={"tp": to}, device_id_type=MESH)
    pl.semaphore_wait(barrier, 4)

    wd, wg, wu = dw_down, dw_gate, dw_up

    def first_phase(dyb, gb, ub):
        def rows_of(g):
            r = rows_at(g * g_rows, g_rows)
            return (
                pltpu.make_async_copy(dy.at[r], dyb, load.at[0]),
                pltpu.make_async_copy(gate.at[r], gb, load.at[1]),
                pltpu.make_async_copy(up.at[r], ub, load.at[2]),
            )

        weights = [pltpu.make_async_copy(a, b, load.at[3 + i]) for i, (a, b) in enumerate(((w_down, wd), (w_gate, wg), (w_up, wu)))]
        weights[0].start()
        for c in rows_of(0):
            c.start()
        weights[1].start()
        weights[2].start()
        weights[0].wait()

        def body(g, _):
            for c in rows_of(g):
                c.wait()
            d_h = dot(dyb[...], wd[...], NT)
            gf, uf = gb[...].astype(F32), ub[...].astype(F32)
            sig = jax.nn.sigmoid(gf)
            silu = gf * sig
            r = rows_at(g * g_rows, g_rows)
            d_all[r, pl.ds(0, ff)] = (d_h * uf * (sig + silu * (1 - sig))).astype(BF)
            d_all[r, pl.ds(ff, ff)] = (d_h * silu).astype(BF)
            hid_t[:, r] = (silu * uf).astype(BF).T

            @pl.when(g < NG - 1)
            def _():
                for c in rows_of(jnp.minimum(g + 1, NG - 1)):
                    c.start()

            @pl.when(g == 0)
            def _():
                weights[1].wait()
                weights[2].wait()

            dg, du = d_all[r, pl.ds(0, ff)], d_all[r, pl.ds(ff, ff)]

            def term(start):
                w = pl.ds(start, half)
                return dot(dg, wg[w, :], NT) + dot(du, wu[w, :], NT)

            @pl.when(g > 0)
            def _():
                c_d2d().wait_send()

            d2d_out[...] = term(other).astype(BF)

            @pl.when(g > 0)
            def _():
                pl.semaphore_wait(credit, 1)

            c_d2d().start()
            acc0[...] = term(mine)
            reduce_events(g)
            e1(g)
            return 0

        lax.fori_loop(0, NG, body, 0)

    pl.run_scoped(
        first_phase,
        pltpu.VMEM((g_rows, wide), BF),
        pltpu.VMEM((g_rows, ff), BF),
        pltpu.VMEM((g_rows, ff), BF),
    )

    def second_phase(xb, yb):
        def loads(i, b):
            c = rows_at(i * cb, cb)
            return (
                pltpu.make_async_copy(x.at[:, c], xb.at[b], load.at[b]),
                pltpu.make_async_copy(dy.at[:, c], yb.at[b], load.at[2 + b]),
            )

        for c in loads(0, 0):
            c.start()

        def early(g, _):
            a0(g)
            return 0

        lax.fori_loop(0, NG - 3, early, 0)

        def body(i, _):
            b = lax.rem(i, 2)

            @pl.when(i < steps - 1)
            def _():
                for c in loads(jnp.minimum(i + 1, steps - 1), 1 - b):
                    c.start()

            into = loads(i, b)
            c = rows_at(i * cb, cb)
            into[0].wait()
            both = dot(xb[b], d_all[...], TN).astype(BF)
            dw_gate[c, :] = both[:, :ff]
            dw_up[c, :] = both[:, ff:]
            slot(2 * i)
            into[1].wait()
            dw_down[:, c] = dot(hid_t[...], yb[b], NN).astype(BF)
            slot(2 * i + 1)
            return 0

        lax.fori_loop(0, steps, body, 0)

    pl.run_scoped(
        second_phase,
        pltpu.VMEM((2, rows, cb), BF),
        pltpu.VMEM((2, rows, cb), BF),
    )

    def rest(s, _):
        slot(s)
        return 0

    lax.fori_loop(2 * steps, last_slot + 1, rest, 0)

    for k in range(3):
        for stage in range(3):
            c_rs(stage, NG - 1, k).wait_send()
    c_d2d().wait_send()

    def drain(g, _):
        for k in range(3):
            c_a0(g, k).wait_send()
            c_a1(g, k).wait_send()
            c_a2(g, k).wait_send()
            c_a3(g, k).wait()
        return 0

    lax.fori_loop(0, NG, drain, 0)


def backward(x, dy, gate, up, w_gate, w_up, w_down, *, cb=512):
    rows, wide = x.shape
    ff = gate.shape[1]
    gr, half = rows // NG, wide // 2
    any_space = pl.BlockSpec(memory_space=pl.ANY)
    dma = pltpu.SemaphoreType.DMA
    grads = pl.pallas_call(
        functools.partial(kernel, cb=cb),
        out_shape=(
            jax.ShapeDtypeStruct((rows, wide), BF),
            pltpu.VMEM((wide, ff), BF),
            pltpu.VMEM((wide, ff), BF),
            pltpu.VMEM((ff, wide), BF),
        ),
        in_specs=[any_space] * 7,
        out_specs=(any_space, *[pl.BlockSpec(memory_space=pltpu.VMEM)] * 3),
        scratch_shapes=[
            pltpu.VMEM((rows, 2 * ff), BF),
            pltpu.VMEM((ff, rows), BF),
            pltpu.VMEM((gr, half), F32),
            pltpu.VMEM((gr // 2, half), F32),
            pltpu.VMEM((gr // 4, half), F32),
            pltpu.VMEM((gr // 8, half), F32),
            pltpu.VMEM((gr, half), BF),
            pltpu.VMEM((gr, half), BF),
            pltpu.VMEM((gr // 2, half), BF),
            pltpu.VMEM((gr // 4, half), BF),
            pltpu.VMEM((gr // 8, half), BF),
            pltpu.VMEM((NG, gr // 2, half), BF),
            pltpu.VMEM((NG, gr // 4, half), BF),
            pltpu.VMEM((NG, gr // 8, half), BF),
            pltpu.VMEM((NG, gr // 8, half), BF),
            dma((6,)),
            dma(()),
            dma(()),
            dma((3,)),
            dma((3,)),
            dma((3,)),
            *[dma((3, NG))] * 3,
            dma((3, NG)),
            *[dma((3, NG))] * 8,
            pltpu.SemaphoreType.REGULAR,
        ],
        compiler_params=pltpu.CompilerParams(
            collective_id=0, has_side_effects=True, vmem_limit_bytes=43_200_000
        ),
        name="mlp_backward",
    )(x, dy, gate, up, w_gate, w_up, w_down)
    return write_out(*grads)


def write_kernel(dx, a, b, c, dx_o, a_o, b_o, c_o, buf, rd, wr, sem):
    slots, piece, _ = buf.shape
    n = dx.shape[0] // piece

    def read(i):
        return pltpu.make_async_copy(dx.at[pl.ds(i * piece, piece)], buf.at[i % slots], rd.at[i % slots])

    def write(i):
        return pltpu.make_async_copy(buf.at[i % slots], dx_o.at[pl.ds(i * piece, piece)], wr.at[i % slots])

    rest = [pltpu.make_async_copy(s, d, sem.at[i]) for i, (s, d) in enumerate(((a, a_o), (b, b_o), (c, c_o)))]
    for i in range(min(slots, n)):
        read(i).start()
    for r in rest:
        r.start()
    for i in range(n):
        read(i).wait()
        write(i).start()
        if i + slots < n:
            write(i).wait()
            read(i + slots).start()
    for i in range(max(n - slots, 0), n):
        write(i).wait()
    for r in rest:
        r.wait()


def write_out(dx, a, b, c, *, pieces=16, slots=8):
    any_space = pl.BlockSpec(memory_space=pl.ANY)
    vmem = pl.BlockSpec(memory_space=pltpu.VMEM)
    dma = pltpu.SemaphoreType.DMA
    rows, wide = dx.shape
    return pl.pallas_call(
        write_kernel,
        out_shape=tuple(jax.ShapeDtypeStruct(r.shape, BF) for r in (dx, a, b, c)),
        in_specs=[any_space, vmem, vmem, vmem],
        out_specs=(any_space,) * 4,
        scratch_shapes=[
            pltpu.VMEM((slots, rows // pieces, wide), BF),
            dma((slots,)),
            dma((slots,)),
            dma((3,)),
        ],
        compiler_params=pltpu.CompilerParams(vmem_limit_bytes=12_000_000),
        name="write_out",
    )(dx, a, b, c)


def solution(mesh):
    tokens, columns, rows = P("dp", None), P(None, "tp"), P("tp", None)
    return jax.shard_map(
        backward,
        mesh=mesh,
        in_specs=(tokens, tokens, P("dp", "tp"), P("dp", "tp"), columns, columns, rows),
        out_specs=(tokens, P("dp", "tp"), P("dp", "tp"), P(("dp", "tp"), None)),
        check_vma=False,
    )
```

```python
import functools

import jax
import jax.numpy as jnp
from jax import lax
from jax.experimental import pallas as pl
from jax.experimental.pallas import tpu as pltpu
from jax.sharding import PartitionSpec as P

MESH = pl.DeviceIdType.MESH
BF, F32 = jnp.bfloat16, jnp.float32
NT = (((1,), (1,)), ((), ()))
TN = (((0,), (0,)), ((), ()))
NN = (((1,), (0,)), ((), ()))
NG = 8
ORDERS = ((8, 4, 2), (4, 2, 8), (2, 8, 4))


def dot(a, b, dims):
    return lax.dot_general(a, b, dims, preferred_element_type=F32)


def colours(half):
    tiles = half // 128
    widths = [128 * ((tiles + 2 - k) // 3) for k in range(3)]
    return [(sum(widths[:k]), widths[k]) for k in range(3)]


def kernel(
    x, dy, gate, up, w_gate, w_up, w_down,
    dx, dw_in, dw_down,
    d_all, hid_t, acc0, acc1, acc2, acc3, d2d_out, d2d_in, out1, out2, out3, in1, in2, in3, fin,
    load, d2d_s, d2d_r, s1, s2, s3, r1, r2, r3, a_loc, a3s, a3r, a2s, a2r, a1s, a1r, ds, dr, credit,
    *, cb,
):
    rows, wide = x.shape
    ff = gate.shape[1]
    g_rows, half = rows // NG, wide // 2
    cols = colours(half)
    steps = wide // cb
    me = lax.axis_index("tp")
    core = lax.rem(me, 2)
    sib = me + 1 - 2 * core
    mine = pl.multiple_of(core * half, 128)
    other = pl.multiple_of((1 - core) * half, 128)

    def stride_of(k, stage):
        first, second = ORDERS[k][stage], ORDERS[(k + 1) % 3][stage]
        return first + core * (second - first)

    def bit(stride):
        return lax.rem(lax.div(me, stride), 2)

    def peer(stride):
        return me + (1 - 2 * bit(stride)) * stride

    def rows_at(start, size):
        return pl.ds(pl.multiple_of(start, size), size)

    def remote(src, dst, send, recv, to):
        return pltpu.make_async_remote_copy(
            src_ref=src, dst_ref=dst, send_sem=send, recv_sem=recv,
            device_id={"tp": to}, device_id_type=MESH,
        )

    def c_d2d():
        return remote(d2d_out, d2d_in, d2d_s, d2d_r, sib)

    def c_rs(stage, g, k):
        src, dst, send, recv = ((out1, in1, s1, r1), (out2, in2, s2, r2), (out3, in3, s3, r3))[stage]
        c = pl.ds(*cols[k])
        return remote(src.at[:, c], dst.at[g, :, c], send.at[k], recv.at[k, g], peer(stride_of(k, stage)))

    def region(g, k, depth):
        start, size = g * g_rows, g_rows
        for stage in range(depth):
            size //= 2
            start = start + bit(stride_of(k, stage)) * size
        return dx.at[rows_at(start, size), pl.ds(pl.multiple_of(mine + cols[k][0], 128), cols[k][1])]

    def c_local(g, k):
        return pltpu.make_async_copy(fin.at[g, :, pl.ds(*cols[k])], region(g, k, 3), a_loc.at[k, g])

    def c_a0(g, k):
        return remote(fin.at[g, :, pl.ds(*cols[k])], region(g, k, 3), a3s.at[k, g], a3r.at[k, g], peer(stride_of(k, 2)))

    def c_a1(g, k):
        return remote(region(g, k, 2), region(g, k, 2), a2s.at[k, g], a2r.at[k, g], peer(stride_of(k, 1)))

    def c_a2(g, k):
        return remote(region(g, k, 1), region(g, k, 1), a1s.at[k, g], a1r.at[k, g], peer(stride_of(k, 0)))

    def c_a3(g, k):
        return remote(region(g, k, 0), region(g, k, 0), ds.at[k, g], dr.at[k, g], sib)

    def e1(g):
        c_d2d().wait_recv()
        h = g_rows // 2
        for k in range(3):
            c = pl.ds(*cols[k])
            away = rows_at((1 - bit(stride_of(k, 0))) * h, h)

            @pl.when(g > 0)
            def _():
                c_rs(0, g, k).wait_send()

            out1[:, c] = (acc0[away, c] + d2d_in[away, c].astype(F32)).astype(BF)
            c_rs(0, g, k).start()
        for k in range(3):
            c = pl.ds(*cols[k])
            keep = rows_at(bit(stride_of(k, 0)) * h, h)
            acc1[:, c] = acc0[keep, c] + d2d_in[keep, c].astype(F32)

        @pl.when(g < NG - 1)
        def _():
            pl.semaphore_signal(credit, inc=1, device_id={"tp": sib}, device_id_type=MESH)

    def e_mid(stage, g, src, came, out, dst):
        h = src.shape[0] // 2
        for k in range(3):
            c = pl.ds(*cols[k])
            c_rs(stage - 1, g, k).wait_recv()
            away = rows_at((1 - bit(stride_of(k, stage))) * h, h)

            @pl.when(g > 0)
            def _():
                c_rs(stage, g, k).wait_send()

            out[:, c] = (src[away, c] + came[g, away, c].astype(F32)).astype(BF)
            c_rs(stage, g, k).start()
            keep = rows_at(bit(stride_of(k, stage)) * h, h)
            dst[:, c] = src[keep, c] + came[g, keep, c].astype(F32)

    def e4(g):
        for k in range(3):
            c = pl.ds(*cols[k])
            c_rs(2, g, k).wait_recv()
            fin[g, :, c] = (acc3[:, c] + in3[g, :, c].astype(F32)).astype(BF)
            c_local(g, k).start()

    def a0(g):
        for k in range(3):
            c_a0(g, k).start()

    def at(cond, f, g):
        @pl.when(cond)
        def _():
            f(g)

    def reduce_events(t):
        at((t >= 3) & (t < NG + 3), e4, t - 3)
        at((t >= 2) & (t < NG + 2), lambda g: e_mid(2, g, acc2, in2, out3, acc3), t - 2)
        at((t >= 1) & (t < NG + 1), lambda g: e_mid(1, g, acc1, in1, out2, acc2), t - 1)

    def a1(g):
        for k in range(3):
            c_local(g, k).wait()
            c_a0(g, k).wait_recv()
            c_a1(g, k).start()

    def a2(g):
        for k in range(3):
            c_a1(g, k).wait_recv()
            c_a2(g, k).start()

    def a3(g):
        for k in range(3):
            c_a2(g, k).wait_recv()
            c_a3(g, k).start()

    def slot(s):
        @pl.when(s < 3)
        def _():
            reduce_events(NG + s)
            at(s >= 0, a0, NG + s - 3)

        for first, num, den, f in ((6, 2, 1, a3), (3, 8, 5, a2), (1, 1, 1, a1)):
            t = den * jnp.maximum(s - first, 0)
            g = lax.div(t, num)
            at((s >= first) & (lax.rem(t, num) < den) & (g < NG), f, g)

    last_slot = 6 + 2 * (NG - 1)

    barrier = pltpu.get_barrier_semaphore()
    for to in (sib, peer(8), peer(4), peer(2)):
        pl.semaphore_signal(barrier, inc=1, device_id={"tp": to}, device_id_type=MESH)

    wd, w_in = dw_down, dw_in

    def first_phase(dyb, gb, ub):
        def rows_of(g):
            r = rows_at(g * g_rows, g_rows)
            return (
                pltpu.make_async_copy(dy.at[r], dyb, load.at[0]),
                pltpu.make_async_copy(gate.at[r], gb, load.at[1]),
                pltpu.make_async_copy(up.at[r], ub, load.at[2]),
            )

        def w_half(start, i):
            r = pl.ds(start, half)
            return [
                pltpu.make_async_copy(w.at[r], w_in.at[r, pl.ds(j * ff, ff)], load.at[4 + 2 * i + j])
                for j, w in enumerate((w_gate, w_up))
            ]

        w_first = pltpu.make_async_copy(w_down, wd, load.at[3])
        w_other, w_mine = w_half(other, 0), w_half(mine, 1)
        for c in (w_first, *rows_of(0), *w_other, *w_mine):
            c.start()
        pl.semaphore_wait(barrier, 4)
        w_first.wait()

        def body(g, _):
            for c in rows_of(g):
                c.wait()
            d_h = dot(dyb[...], wd[...], NT)
            gf, uf = gb[...].astype(F32), ub[...].astype(F32)
            sig = jax.nn.sigmoid(gf)
            silu = gf * sig
            r = rows_at(g * g_rows, g_rows)
            d_all[r, pl.ds(0, ff)] = (d_h * uf * (sig + silu * (1 - sig))).astype(BF)
            d_all[r, pl.ds(ff, ff)] = (d_h * silu).astype(BF)
            hid_t[:, r] = (silu * uf).astype(BF).T

            @pl.when(g < NG - 1)
            def _():
                for c in rows_of(jnp.minimum(g + 1, NG - 1)):
                    c.start()

            def when_first(copies):
                @pl.when(g == 0)
                def _():
                    for c in copies:
                        c.wait()

            def term(start):
                return dot(d_all[r, :], w_in[pl.ds(start, half), :], NT)

            when_first(w_other)

            @pl.when(g > 0)
            def _():
                c_d2d().wait_send()

            d2d_out[...] = term(other).astype(BF)

            @pl.when(g > 0)
            def _():
                pl.semaphore_wait(credit, 1)

            c_d2d().start()
            when_first(w_mine)
            acc0[...] = term(mine)
            reduce_events(g)
            e1(g)
            return 0

        lax.fori_loop(0, NG, body, 0)

    pl.run_scoped(
        first_phase,
        pltpu.VMEM((g_rows, wide), BF),
        pltpu.VMEM((g_rows, ff), BF),
        pltpu.VMEM((g_rows, ff), BF),
    )

    def second_phase(xb, yb):
        def loads(i, b):
            c = rows_at(i * cb, cb)
            return (
                pltpu.make_async_copy(x.at[:, c], xb.at[b], load.at[b]),
                pltpu.make_async_copy(dy.at[:, c], yb.at[b], load.at[2 + b]),
            )

        for c in loads(0, 0):
            c.start()

        def early(g, _):
            a0(g)
            return 0

        lax.fori_loop(0, NG - 3, early, 0)

        def body(i, _):
            b = lax.rem(i, 2)

            @pl.when(i < steps - 1)
            def _():
                for c in loads(jnp.minimum(i + 1, steps - 1), 1 - b):
                    c.start()

            into = loads(i, b)
            c = rows_at(i * cb, cb)
            into[0].wait()
            dw_in[c, :] = dot(xb[b], d_all[...], TN).astype(BF)
            slot(2 * i)
            into[1].wait()
            dw_down[:, c] = dot(hid_t[...], yb[b], NN).astype(BF)
            slot(2 * i + 1)
            return 0

        lax.fori_loop(0, steps, body, 0)

    pl.run_scoped(
        second_phase,
        pltpu.VMEM((2, rows, cb), BF),
        pltpu.VMEM((2, rows, cb), BF),
    )

    def rest(s, _):
        slot(s)
        return 0

    lax.fori_loop(2 * steps, last_slot + 1, rest, 0)

    for k in range(3):
        for stage in range(3):
            c_rs(stage, NG - 1, k).wait_send()
    c_d2d().wait_send()

    def drain(g, _):
        for k in range(3):
            c_a0(g, k).wait_send()
            c_a1(g, k).wait_send()
            c_a2(g, k).wait_send()
            c_a3(g, k).wait()
        return 0

    lax.fori_loop(0, NG, drain, 0)


def backward(x, dy, gate, up, w_gate, w_up, w_down, *, cb=512):
    rows, wide = x.shape
    ff = gate.shape[1]
    gr, half = rows // NG, wide // 2
    any_space = pl.BlockSpec(memory_space=pl.ANY)
    dma = pltpu.SemaphoreType.DMA
    grads = pl.pallas_call(
        functools.partial(kernel, cb=cb),
        out_shape=(
            jax.ShapeDtypeStruct((rows, wide), BF),
            pltpu.VMEM((wide, 2 * ff), BF),
            pltpu.VMEM((ff, wide), BF),
        ),
        in_specs=[any_space] * 7,
        out_specs=(any_space, *[pl.BlockSpec(memory_space=pltpu.VMEM)] * 2),
        scratch_shapes=[
            pltpu.VMEM((rows, 2 * ff), BF),
            pltpu.VMEM((ff, rows), BF),
            pltpu.VMEM((gr, half), F32),
            pltpu.VMEM((gr // 2, half), F32),
            pltpu.VMEM((gr // 4, half), F32),
            pltpu.VMEM((gr // 8, half), F32),
            pltpu.VMEM((gr, half), BF),
            pltpu.VMEM((gr, half), BF),
            pltpu.VMEM((gr // 2, half), BF),
            pltpu.VMEM((gr // 4, half), BF),
            pltpu.VMEM((gr // 8, half), BF),
            pltpu.VMEM((NG, gr // 2, half), BF),
            pltpu.VMEM((NG, gr // 4, half), BF),
            pltpu.VMEM((NG, gr // 8, half), BF),
            pltpu.VMEM((NG, gr // 8, half), BF),
            dma((8,)),
            dma(()),
            dma(()),
            dma((3,)),
            dma((3,)),
            dma((3,)),
            *[dma((3, NG))] * 3,
            dma((3, NG)),
            *[dma((3, NG))] * 8,
            pltpu.SemaphoreType.REGULAR,
        ],
        compiler_params=pltpu.CompilerParams(
            collective_id=0, has_side_effects=True, vmem_limit_bytes=43_200_000
        ),
        name="mlp_backward",
    )(x, dy, gate, up, w_gate, w_up, w_down)
    return write_out(*grads)


def write_kernel(dx, ab, c, dx_o, a_o, b_o, c_o, buf, rd, wr, sem):
    slots, piece, _ = buf.shape
    n = dx.shape[0] // piece

    def read(i):
        return pltpu.make_async_copy(dx.at[pl.ds(i * piece, piece)], buf.at[i % slots], rd.at[i % slots])

    def write(i):
        return pltpu.make_async_copy(buf.at[i % slots], dx_o.at[pl.ds(i * piece, piece)], wr.at[i % slots])

    ff = a_o.shape[1]
    parts = ((ab.at[:, pl.ds(0, ff)], a_o), (ab.at[:, pl.ds(ff, ff)], b_o), (c, c_o))
    rest = [pltpu.make_async_copy(s, d, sem.at[i]) for i, (s, d) in enumerate(parts)]
    for i in range(min(slots, n)):
        read(i).start()
    for r in rest:
        r.start()
    for i in range(n):
        read(i).wait()
        write(i).start()
        if i + slots < n:
            write(i).wait()
            read(i + slots).start()
    for i in range(max(n - slots, 0), n):
        write(i).wait()
    for r in rest:
        r.wait()


def write_out(dx, ab, c, *, pieces=16, slots=8):
    any_space = pl.BlockSpec(memory_space=pl.ANY)
    vmem = pl.BlockSpec(memory_space=pltpu.VMEM)
    dma = pltpu.SemaphoreType.DMA
    rows, wide = dx.shape
    ff = c.shape[0]
    return pl.pallas_call(
        write_kernel,
        out_shape=tuple(jax.ShapeDtypeStruct(r, BF) for r in (dx.shape, (wide, ff), (wide, ff), c.shape)),
        in_specs=[any_space, vmem, vmem],
        out_specs=(any_space,) * 4,
        scratch_shapes=[
            pltpu.VMEM((slots, rows // pieces, wide), BF),
            dma((slots,)),
            dma((slots,)),
            dma((3,)),
        ],
        compiler_params=pltpu.CompilerParams(vmem_limit_bytes=12_000_000),
        name="write_out",
    )(dx, ab, c)


def solution(mesh):
    tokens, columns, rows = P("dp", None), P(None, "tp"), P("tp", None)
    return jax.shard_map(
        backward,
        mesh=mesh,
        in_specs=(tokens, tokens, P("dp", "tp"), P("dp", "tp"), columns, columns, rows),
        out_specs=(tokens, P("dp", "tp"), P("dp", "tp"), P(("dp", "tp"), None)),
        check_vma=False,
    )
```

```python
import functools

import jax
import jax.numpy as jnp
from jax import lax
from jax.experimental import pallas as pl
from jax.experimental.pallas import tpu as pltpu
from jax.sharding import PartitionSpec as P

MESH = pl.DeviceIdType.MESH
BF, F32 = jnp.bfloat16, jnp.float32
NT = (((1,), (1,)), ((), ()))
TN = (((0,), (0,)), ((), ()))
NN = (((1,), (0,)), ((), ()))
NG = 8
ORDERS = ((8, 4, 2), (4, 2, 8), (2, 8, 4))


def dot(a, b, dims):
    return lax.dot_general(a, b, dims, preferred_element_type=F32)


def colours(half):
    tiles = half // 128
    widths = [128 * ((tiles + 2 - k) // 3) for k in range(3)]
    return [(sum(widths[:k]), widths[k]) for k in range(3)]


def kernel(
    x, dy, gate, up, w_gate, w_up, w_down,
    dx, dw_gate, dw_up, dw_down, d_kept, hid_kept,
    acc1, acc2, acc3, d2d_out, out1, out2, out3,
    load, d2d_s, d2d_r, s1, s2, s3, r1, r2, r3, a3s, a3r, a2s, a2r, a1s, a1r, ds, dr, credit,
    *, cb,
):
    rows, wide = x.shape
    ff = gate.shape[1]
    g_rows, half = rows // NG, wide // 2
    cols = colours(half)
    steps = wide // cb
    me = lax.axis_index("tp")
    core = lax.rem(me, 2)
    sib = me + 1 - 2 * core
    mine = pl.multiple_of(core * half, 128)
    other = pl.multiple_of((1 - core) * half, 128)

    def stride_of(k, stage):
        first, second = ORDERS[k][stage], ORDERS[(k + 1) % 3][stage]
        return first + core * (second - first)

    def bit(stride):
        return lax.rem(lax.div(me, stride), 2)

    def peer(stride):
        return me + (1 - 2 * bit(stride)) * stride

    def rows_at(start, size):
        return pl.ds(pl.multiple_of(start, size), size)

    def remote(src, dst, send, recv, to):
        return pltpu.make_async_remote_copy(
            src_ref=src, dst_ref=dst, send_sem=send, recv_sem=recv,
            device_id={"tp": to}, device_id_type=MESH,
        )

    def own(g, k, start, size):
        return rows_at(start + g * g_rows, size), pl.ds(pl.multiple_of(mine + cols[k][0], 128), cols[k][1])

    def landing(g, k, stage, b):
        h = g_rows // 2
        start, size = ((b * h, h), ((1 - b) * h, h // 2), ((1 - b) * h + h // 2, h // 4))[stage]
        return start, size

    def came(g, k, stage, start, size):
        first, _ = landing(g, k, stage, bit(stride_of(k, 0)))
        return dx[own(g, k, first + start, size)].astype(F32)

    def c_d2d(g):
        return remote(d2d_out, dx.at[rows_at(g * g_rows, g_rows), pl.ds(mine, half)], d2d_s, d2d_r.at[g], sib)

    def c_rs(stage, g, k):
        src, send, recv = ((out1, s1, r1), (out2, s2, r2), (out3, s3, r3))[stage]
        b = bit(stride_of(k, 0))
        dst = own(g, k, *landing(g, k, stage, 1 - b if stage == 0 else b))
        return remote(src.at[:, pl.ds(*cols[k])], dx.at[dst], send.at[k], recv.at[k, g], peer(stride_of(k, stage)))

    def held(k, depth):
        start, size = 0, g_rows
        for stage in range(depth):
            size //= 2
            start = start + bit(stride_of(k, stage)) * size
        return start, size

    def region(g, k, depth):
        return dx.at[own(g, k, *held(k, depth))]

    def c_a0(g, k):
        return remote(region(g, k, 3), region(g, k, 3), a3s.at[k, g], a3r.at[k, g], peer(stride_of(k, 2)))

    def c_a1(g, k):
        return remote(region(g, k, 2), region(g, k, 2), a2s.at[k, g], a2r.at[k, g], peer(stride_of(k, 1)))

    def c_a2(g, k):
        return remote(region(g, k, 1), region(g, k, 1), a1s.at[k, g], a1r.at[k, g], peer(stride_of(k, 0)))

    def c_a3(g, k):
        return remote(region(g, k, 0), region(g, k, 0), ds.at[k, g], dr.at[k, g], sib)

    def e1(g, acc0):
        c_d2d(g).wait_recv()
        h = g_rows // 2

        def chip_sum(k, start):
            theirs = dx[rows_at(g * g_rows + start, h), pl.ds(pl.multiple_of(other + cols[k][0], 128), cols[k][1])]
            return acc0[rows_at(start, h), pl.ds(*cols[k])] + theirs.astype(F32)

        for k in range(3):

            @pl.when(g > 0)
            def _():
                c_rs(0, g, k).wait_send()

            out1[:, pl.ds(*cols[k])] = chip_sum(k, (1 - bit(stride_of(k, 0))) * h).astype(BF)
            c_rs(0, g, k).start()
        for k in range(3):
            acc1[:, pl.ds(*cols[k])] = chip_sum(k, bit(stride_of(k, 0)) * h)

    def e_mid(stage, g, src, out, dst):
        h = src.shape[0] // 2
        for k in range(3):
            c = pl.ds(*cols[k])
            c_rs(stage - 1, g, k).wait_recv()
            away = (1 - bit(stride_of(k, stage))) * h
            keep = bit(stride_of(k, stage)) * h

            @pl.when(g > 0)
            def _():
                c_rs(stage, g, k).wait_send()

            out[:, c] = (src[rows_at(away, h), c] + came(g, k, stage - 1, away, h)).astype(BF)
            c_rs(stage, g, k).start()
            dst[:, c] = src[rows_at(keep, h), c] + came(g, k, stage - 1, keep, h)

    def e4(g):
        for k in range(3):
            c_rs(2, g, k).wait_recv()
            size = acc3.shape[0]
            total = acc3[:, pl.ds(*cols[k])] + came(g, k, 2, 0, size)
            dx[own(g, k, *held(k, 3))] = total.astype(BF)

    def a0(g):
        for k in range(3):
            c_a0(g, k).start()

    def at(cond, f, g):
        @pl.when(cond)
        def _():
            f(g)

    def reduce_events(t):
        at((t >= 3) & (t < NG + 3), e4, t - 3)
        at((t >= 2) & (t < NG + 2), lambda g: e_mid(2, g, acc2, out3, acc3), t - 2)
        at((t >= 1) & (t < NG + 1), lambda g: e_mid(1, g, acc1, out2, acc2), t - 1)

    def a1(g):
        for k in range(3):
            c_a0(g, k).wait_recv()
            c_a1(g, k).start()

    def a2(g):
        for k in range(3):
            c_a1(g, k).wait_recv()
            c_a2(g, k).start()

    def a3(g):
        for k in range(3):
            c_a2(g, k).wait_recv()
            c_a3(g, k).start()

    def slot(s):
        @pl.when(s < 3)
        def _():
            reduce_events(NG + s)
            at(s >= 0, a0, NG + s - 3)

        @pl.when(s == 2)
        def _():
            for to in (sib, peer(8), peer(4), peer(2)):
                pl.semaphore_signal(credit, inc=1, device_id={"tp": to}, device_id_type=MESH)

        @pl.when(s == 3)
        def _():
            pl.semaphore_wait(credit, 4)

        for first, num, den, f in ((6, 2, 1, a3), (3, 8, 5, a2), (1, 1, 1, a1)):
            t = den * jnp.maximum(s - first, 0)
            g = lax.div(t, num)
            at((s >= first) & (lax.rem(t, num) < den) & (g < NG), f, g)

    last_slot = 6 + 2 * (NG - 1)

    barrier = pltpu.get_barrier_semaphore()
    for to in (sib, peer(8), peer(4), peer(2)):
        pl.semaphore_signal(barrier, inc=1, device_id={"tp": to}, device_id_type=MESH)

    wd, wg, wu = dw_down, dw_gate, dw_up

    def first_phase(acc0, dyb, gb, ub, d_in, hid):
        def rows_of(g):
            r = rows_at(g * g_rows, g_rows)
            return (
                pltpu.make_async_copy(dy.at[r], dyb, load.at[0]),
                pltpu.make_async_copy(gate.at[r], gb, load.at[1]),
                pltpu.make_async_copy(up.at[r], ub, load.at[2]),
            )

        def keep(g):
            r = rows_at(g * g_rows, g_rows)
            return (
                pltpu.make_async_copy(d_in, d_kept.at[r], load.at[8]),
                pltpu.make_async_copy(hid, hid_kept.at[:, r], load.at[9]),
            )

        def w_half(start, i):
            r = pl.ds(start, half)
            return [
                pltpu.make_async_copy(w.at[r], v.at[r], load.at[4 + 2 * i + j])
                for j, (w, v) in enumerate(((w_gate, wg), (w_up, wu)))
            ]

        w_first = pltpu.make_async_copy(w_down, wd, load.at[3])
        w_other, w_mine = w_half(other, 0), w_half(mine, 1)
        for c in (w_first, *rows_of(0), *w_other, *w_mine):
            c.start()
        pl.semaphore_wait(barrier, 4)
        w_first.wait()

        def body(g, _):
            for c in rows_of(g):
                c.wait()
            @pl.when(g < NG)
            def _():
                acc0[:, pl.ds(0, ff)] = dot(dyb[...], wd[...], NT)

            d_h = acc0[:, pl.ds(0, ff)]
            gf, uf = gb[...].astype(F32), ub[...].astype(F32)
            sig = jax.nn.sigmoid(gf)
            silu = gf * sig

            @pl.when(g > 0)
            def _():
                for c in keep(g):
                    c.wait()

            d_in[:, pl.ds(0, ff)] = (d_h * uf * (sig + silu * (1 - sig))).astype(BF)
            d_in[:, pl.ds(ff, ff)] = (d_h * silu).astype(BF)
            hid[...] = (silu * uf).astype(BF).T
            for c in keep(g):
                c.start()

            @pl.when(g < NG - 1)
            def _():
                for c in rows_of(jnp.minimum(g + 1, NG - 1)):
                    c.start()

            def when_first(copies):
                @pl.when(g == 0)
                def _():
                    for c in copies:
                        c.wait()

            def term(start):
                w = pl.ds(start, half)
                return dot(d_in[:, pl.ds(0, ff)], wg[w, :], NT) + dot(d_in[:, pl.ds(ff, ff)], wu[w, :], NT)

            when_first(w_other)

            @pl.when(g > 0)
            def _():
                c_d2d(g).wait_send()

            @pl.when(g < NG)
            def _():
                acc0[...] = term(other)

            d2d_out[...] = acc0[...].astype(BF)

            c_d2d(g).start()
            when_first(w_mine)
            @pl.when(g < NG)
            def _():
                acc0[...] = term(mine)

            reduce_events(g)
            e1(g, acc0)
            return 0

        lax.fori_loop(0, NG, body, 0)
        for c in keep(NG - 1):
            c.wait()

    pl.run_scoped(
        first_phase,
        pltpu.VMEM((g_rows, half), F32),
        pltpu.VMEM((g_rows, wide), BF),
        pltpu.VMEM((g_rows, ff), BF),
        pltpu.VMEM((g_rows, ff), BF),
        pltpu.VMEM((g_rows, 2 * ff), BF),
        pltpu.VMEM((ff, g_rows), BF),
    )

    def second_phase(d_all, hid_t, xb, yb):
        again = (pltpu.make_async_copy(d_kept, d_all, load.at[8]), pltpu.make_async_copy(hid_kept, hid_t, load.at[9]))
        for c in again:
            c.start()

        def loads(i, b):
            c = rows_at(i * cb, cb)
            return (
                pltpu.make_async_copy(x.at[:, c], xb.at[b], load.at[b]),
                pltpu.make_async_copy(dy.at[:, c], yb.at[b], load.at[2 + b]),
            )

        for c in loads(0, 0):
            c.start()

        def early(g, _):
            a0(g)
            return 0

        lax.fori_loop(0, NG - 3, early, 0)
        for c in again:
            c.wait()

        def body(i, _):
            b = lax.rem(i, 2)

            @pl.when(i < steps - 1)
            def _():
                for c in loads(jnp.minimum(i + 1, steps - 1), 1 - b):
                    c.start()

            into = loads(i, b)
            c = rows_at(i * cb, cb)
            into[0].wait()

            @pl.when(i < steps)
            def _():
                both = dot(xb[b], d_all[...], TN).astype(BF)
                dw_gate[c, :] = both[:, :ff]
                dw_up[c, :] = both[:, ff:]

            into[1].wait()

            @pl.when(i < steps)
            def _():
                dw_down[:, c] = dot(hid_t[...], yb[b], NN).astype(BF)

            slot(i)
            return 0

        lax.fori_loop(0, steps, body, 0)

    pl.run_scoped(
        second_phase,
        pltpu.VMEM((rows, 2 * ff), BF),
        pltpu.VMEM((ff, rows), BF),
        pltpu.VMEM((2, rows, cb), BF),
        pltpu.VMEM((2, rows, cb), BF),
    )

    def rest(s, _):
        slot(s)
        return 0

    lax.fori_loop(steps, last_slot + 1, rest, 0)

    for k in range(3):
        for stage in range(3):
            c_rs(stage, NG - 1, k).wait_send()
    c_d2d(NG - 1).wait_send()

    def drain(g, _):
        for k in range(3):
            c_a0(g, k).wait_send()
            c_a1(g, k).wait_send()
            c_a2(g, k).wait_send()
            c_a3(g, k).wait()
        return 0

    lax.fori_loop(0, NG, drain, 0)


def backward(x, dy, gate, up, w_gate, w_up, w_down, *, cb=256):
    rows, wide = x.shape
    ff = gate.shape[1]
    gr, half = rows // NG, wide // 2
    any_space = pl.BlockSpec(memory_space=pl.ANY)
    dma = pltpu.SemaphoreType.DMA
    grads = pl.pallas_call(
        functools.partial(kernel, cb=cb),
        out_shape=(
            pltpu.VMEM((rows, wide), BF),
            pltpu.VMEM((wide, ff), BF),
            pltpu.VMEM((wide, ff), BF),
            pltpu.VMEM((ff, wide), BF),
            jax.ShapeDtypeStruct((rows, 2 * ff), BF),
            jax.ShapeDtypeStruct((ff, rows), BF),
        ),
        in_specs=[any_space] * 7,
        out_specs=(*[pl.BlockSpec(memory_space=pltpu.VMEM)] * 4, any_space, any_space),
        scratch_shapes=[
            pltpu.VMEM((gr // 2, half), F32),
            pltpu.VMEM((gr // 4, half), F32),
            pltpu.VMEM((gr // 8, half), F32),
            pltpu.VMEM((gr, half), BF),
            pltpu.VMEM((gr // 2, half), BF),
            pltpu.VMEM((gr // 4, half), BF),
            pltpu.VMEM((gr // 8, half), BF),
            dma((10,)),
            dma(()),
            dma((NG,)),
            dma((3,)),
            dma((3,)),
            dma((3,)),
            *[dma((3, NG))] * 3,
            *[dma((3, NG))] * 8,
            pltpu.SemaphoreType.REGULAR,
        ],
        compiler_params=pltpu.CompilerParams(
            collective_id=0, has_side_effects=True, vmem_limit_bytes=22_400_000
        ),
        name="mlp_backward",
    )(x, dy, gate, up, w_gate, w_up, w_down)
    return grads[:4]


def solution(mesh):
    tokens, columns, rows = P("dp", None), P(None, "tp"), P("tp", None)
    return jax.shard_map(
        backward,
        mesh=mesh,
        in_specs=(tokens, tokens, P("dp", "tp"), P("dp", "tp"), columns, columns, rows),
        out_specs=(tokens, P("dp", "tp"), P("dp", "tp"), P(("dp", "tp"), None)),
        check_vma=False,
    )
```

```python
import functools

import jax
import jax.numpy as jnp
from jax import lax
from jax.experimental import pallas as pl
from jax.experimental.pallas import tpu as pltpu
from jax.sharding import PartitionSpec as P

MESH = pl.DeviceIdType.MESH
BF, F32 = jnp.bfloat16, jnp.float32
NT = (((1,), (1,)), ((), ()))
TN = (((0,), (0,)), ((), ()))
NN = (((1,), (0,)), ((), ()))
NG = 8
ORDERS = ((8, 4, 2), (4, 2, 8), (2, 8, 4))


def dot(a, b, dims):
    return lax.dot_general(a, b, dims, preferred_element_type=F32)


def colours(half):
    tiles = half // 128
    widths = [128 * ((tiles + 2 - k) // 3) for k in range(3)]
    return [(sum(widths[:k]), widths[k]) for k in range(3)]


def kernel(
    x, dy, gate, up, w_gate, w_up, w_down,
    dx, dw_gate, dw_up, dw_down, d_kept, hid_kept,
    acc1, acc2, acc3, d2d_out, out1, out2, out3,
    load, d2d_s, d2d_r, s1, s2, s3, r1, r2, r3, a3s, a3r, a2s, a2r, a1s, a1r, ds, dr, credit,
    *, cb,
):
    rows, wide = x.shape
    ff = gate.shape[1]
    g_rows, half = rows // NG, wide // 2
    cols = colours(half)
    steps = wide // cb
    me = lax.axis_index("tp")
    core = lax.rem(me, 2)
    sib = me + 1 - 2 * core
    mine = pl.multiple_of(core * half, 128)
    other = pl.multiple_of((1 - core) * half, 128)

    def stride_of(k, stage):
        first, second = ORDERS[k][stage], ORDERS[(k + 1) % 3][stage]
        return first + core * (second - first)

    def bit(stride):
        return lax.rem(lax.div(me, stride), 2)

    def peer(stride):
        return me + (1 - 2 * bit(stride)) * stride

    def rows_at(start, size):
        return pl.ds(pl.multiple_of(start, size), size)

    def remote(src, dst, send, recv, to):
        return pltpu.make_async_remote_copy(
            src_ref=src, dst_ref=dst, send_sem=send, recv_sem=recv,
            device_id={"tp": to}, device_id_type=MESH,
        )

    def own(g, k, start, size):
        return rows_at(start + g * g_rows, size), pl.ds(pl.multiple_of(mine + cols[k][0], 128), cols[k][1])

    def landing(g, k, stage, b):
        h = g_rows // 2
        start, size = ((b * h, h), ((1 - b) * h, h // 2), ((1 - b) * h + h // 2, h // 4))[stage]
        return start, size

    def came(g, k, stage, start, size):
        first, _ = landing(g, k, stage, bit(stride_of(k, 0)))
        return dx[own(g, k, first + start, size)].astype(F32)

    def c_d2d(g):
        return remote(d2d_out, dx.at[rows_at(g * g_rows, g_rows), pl.ds(mine, half)], d2d_s, d2d_r.at[g], sib)

    def c_rs(stage, g, k):
        src, send, recv = ((out1, s1, r1), (out2, s2, r2), (out3, s3, r3))[stage]
        b = bit(stride_of(k, 0))
        dst = own(g, k, *landing(g, k, stage, 1 - b if stage == 0 else b))
        return remote(src.at[:, pl.ds(*cols[k])], dx.at[dst], send.at[k], recv.at[k, g], peer(stride_of(k, stage)))

    def held(k, depth):
        start, size = 0, g_rows
        for stage in range(depth):
            size //= 2
            start = start + bit(stride_of(k, stage)) * size
        return start, size

    def region(g, k, depth):
        return dx.at[own(g, k, *held(k, depth))]

    def c_a0(g, k):
        return remote(region(g, k, 3), region(g, k, 3), a3s.at[k, g], a3r.at[k, g], peer(stride_of(k, 2)))

    def c_a1(g, k):
        return remote(region(g, k, 2), region(g, k, 2), a2s.at[k, g], a2r.at[k, g], peer(stride_of(k, 1)))

    def c_a2(g, k):
        return remote(region(g, k, 1), region(g, k, 1), a1s.at[k, g], a1r.at[k, g], peer(stride_of(k, 0)))

    def c_a3(g, k, late):
        start, size = held(k, 1)
        rows_to = dx.at[own(g, k, size - start if late else start, size)]
        return remote(rows_to, rows_to, ds.at[late, k, g], dr.at[late, k, g], sib)

    def e1(g, acc0):
        c_d2d(g).wait_recv()
        h = g_rows // 2

        def chip_sum(k, start):
            theirs = dx[rows_at(g * g_rows + start, h), pl.ds(pl.multiple_of(other + cols[k][0], 128), cols[k][1])]
            return acc0[rows_at(start, h), pl.ds(*cols[k])] + theirs.astype(F32)

        for k in range(3):

            @pl.when(g > 0)
            def _():
                c_rs(0, g, k).wait_send()

            out1[:, pl.ds(*cols[k])] = chip_sum(k, (1 - bit(stride_of(k, 0))) * h).astype(BF)
            c_rs(0, g, k).start()
        for k in range(3):
            acc1[:, pl.ds(*cols[k])] = chip_sum(k, bit(stride_of(k, 0)) * h)

    def e_mid(stage, g, src, out, dst):
        h = src.shape[0] // 2
        for k in range(3):
            c = pl.ds(*cols[k])
            c_rs(stage - 1, g, k).wait_recv()
            away = (1 - bit(stride_of(k, stage))) * h
            keep = bit(stride_of(k, stage)) * h

            @pl.when(g > 0)
            def _():
                c_rs(stage, g, k).wait_send()

            out[:, c] = (src[rows_at(away, h), c] + came(g, k, stage - 1, away, h)).astype(BF)
            c_rs(stage, g, k).start()
            dst[:, c] = src[rows_at(keep, h), c] + came(g, k, stage - 1, keep, h)

    def e4(g):
        for k in range(3):
            c_rs(2, g, k).wait_recv()
            size = acc3.shape[0]
            total = acc3[:, pl.ds(*cols[k])] + came(g, k, 2, 0, size)
            dx[own(g, k, *held(k, 3))] = total.astype(BF)

    def a0(g):
        for k in range(3):
            c_a0(g, k).start()

    def at(cond, f, g):
        @pl.when(cond)
        def _():
            f(g)

    def reduce_events(t):
        at((t >= 3) & (t < NG + 3), e4, t - 3)
        at((t >= 2) & (t < NG + 2), lambda g: e_mid(2, g, acc2, out3, acc3), t - 2)
        at((t >= 1) & (t < NG + 1), lambda g: e_mid(1, g, acc1, out2, acc2), t - 1)

    def a1(g):
        for k in range(3):
            c_a0(g, k).wait_recv()
            c_a1(g, k).start()

    def a2(g):
        for k in range(3):
            c_a1(g, k).wait_recv()
            c_a2(g, k).start()
        for k in range(3):
            c_a3(g, k, 0).start()

    def a3(g):
        for k in range(3):
            c_a2(g, k).wait_recv()
            c_a3(g, k, 1).start()

    def slot(s):
        @pl.when(s < 3)
        def _():
            reduce_events(NG + s)
            at(s >= 0, a0, NG + s - 3)

        @pl.when(s == 2)
        def _():
            for to in (sib, peer(8), peer(4), peer(2)):
                pl.semaphore_signal(credit, inc=1, device_id={"tp": to}, device_id_type=MESH)

        @pl.when(s == 3)
        def _():
            pl.semaphore_wait(credit, 4)

        for first, num, den, f in ((7, 9, 5, a3), (3, 3, 2, a2), (1, 1, 1, a1)):
            t = den * jnp.maximum(s - first, 0)
            g = lax.div(t, num)
            at((s >= first) & (lax.rem(t, num) < den) & (g < NG), f, g)

    last_slot = 7 + (9 * (NG - 1) + 4) // 5

    barrier = pltpu.get_barrier_semaphore()
    for to in (sib, peer(8), peer(4), peer(2)):
        pl.semaphore_signal(barrier, inc=1, device_id={"tp": to}, device_id_type=MESH)

    wd, wg, wu = dw_down, dw_gate, dw_up

    def first_phase(acc0, dyb, gb, ub, d_in, hid):
        def rows_of(g):
            r = rows_at(g * g_rows, g_rows)
            return (
                pltpu.make_async_copy(dy.at[r], dyb, load.at[0]),
                pltpu.make_async_copy(gate.at[r], gb, load.at[1]),
                pltpu.make_async_copy(up.at[r], ub, load.at[2]),
            )

        def keep(g):
            r = rows_at(g * g_rows, g_rows)
            return (
                pltpu.make_async_copy(d_in, d_kept.at[r], load.at[8]),
                pltpu.make_async_copy(hid, hid_kept.at[:, r], load.at[9]),
            )

        def w_half(start, i):
            r = pl.ds(start, half)
            return [
                pltpu.make_async_copy(w.at[r], v.at[r], load.at[4 + 2 * i + j])
                for j, (w, v) in enumerate(((w_gate, wg), (w_up, wu)))
            ]

        w_first = pltpu.make_async_copy(w_down, wd, load.at[3])
        w_other, w_mine = w_half(other, 0), w_half(mine, 1)
        for c in (w_first, *rows_of(0), *w_other, *w_mine):
            c.start()
        pl.semaphore_wait(barrier, 4)
        w_first.wait()

        def body(g, _):
            for c in rows_of(g):
                c.wait()

            @pl.when(g > 0)
            def _():
                for c in keep(g):
                    c.wait()
            @pl.when(g < NG)
            def _():
                acc0[:, pl.ds(0, ff)] = dot(dyb[...], wd[...], NT)

            d_h = acc0[:, pl.ds(0, ff)]
            gf, uf = gb[...].astype(F32), ub[...].astype(F32)
            sig = jax.nn.sigmoid(gf)
            silu = gf * sig

            d_in[:, pl.ds(0, ff)] = (d_h * uf * (sig + silu * (1 - sig))).astype(BF)
            d_in[:, pl.ds(ff, ff)] = (d_h * silu).astype(BF)
            hid[...] = (silu * uf).astype(BF).T
            for c in keep(g):
                c.start()

            @pl.when(g < NG - 1)
            def _():
                for c in rows_of(jnp.minimum(g + 1, NG - 1)):
                    c.start()

            def when_first(copies):
                @pl.when(g == 0)
                def _():
                    for c in copies:
                        c.wait()

            def term(start):
                w = pl.ds(start, half)
                return dot(d_in[:, pl.ds(0, ff)], wg[w, :], NT) + dot(d_in[:, pl.ds(ff, ff)], wu[w, :], NT)

            when_first(w_other)

            @pl.when(g > 0)
            def _():
                c_d2d(g).wait_send()

            @pl.when(g < NG)
            def _():
                acc0[...] = term(other)

            d2d_out[...] = acc0[...].astype(BF)

            c_d2d(g).start()
            reduce_events(g)
            when_first(w_mine)
            @pl.when(g < NG)
            def _():
                acc0[...] = term(mine)

            e1(g, acc0)
            return 0

        lax.fori_loop(0, NG, body, 0)
        for c in keep(NG - 1):
            c.wait()

    pl.run_scoped(
        first_phase,
        pltpu.VMEM((g_rows, half), F32),
        pltpu.VMEM((g_rows, wide), BF),
        pltpu.VMEM((g_rows, ff), BF),
        pltpu.VMEM((g_rows, ff), BF),
        pltpu.VMEM((g_rows, 2 * ff), BF),
        pltpu.VMEM((ff, g_rows), BF),
    )

    def second_phase(d_all, hid_t, xb, yb):
        again = (pltpu.make_async_copy(d_kept, d_all, load.at[8]), pltpu.make_async_copy(hid_kept, hid_t, load.at[9]))
        for c in again:
            c.start()

        def loads(i, b):
            c = rows_at(i * cb, cb)
            return (
                pltpu.make_async_copy(x.at[:, c], xb.at[b], load.at[b]),
                pltpu.make_async_copy(dy.at[:, c], yb.at[b], load.at[2 + b]),
            )

        for c in loads(0, 0):
            c.start()

        def early(g, _):
            a0(g)
            return 0

        lax.fori_loop(0, NG - 3, early, 0)
        for c in again:
            c.wait()

        def body(i, _):
            b = lax.rem(i, 2)

            @pl.when(i < steps - 1)
            def _():
                for c in loads(jnp.minimum(i + 1, steps - 1), 1 - b):
                    c.start()

            into = loads(i, b)
            c = rows_at(i * cb, cb)
            into[0].wait()

            @pl.when(i < steps)
            def _():
                both = dot(xb[b], d_all[...], TN).astype(BF)
                dw_gate[c, :] = both[:, :ff]
                dw_up[c, :] = both[:, ff:]

            into[1].wait()

            @pl.when(i < steps)
            def _():
                dw_down[:, c] = dot(hid_t[...], yb[b], NN).astype(BF)

            slot(i)
            return 0

        lax.fori_loop(0, steps, body, 0)

    pl.run_scoped(
        second_phase,
        pltpu.VMEM((rows, 2 * ff), BF),
        pltpu.VMEM((ff, rows), BF),
        pltpu.VMEM((2, rows, cb), BF),
        pltpu.VMEM((2, rows, cb), BF),
    )

    def rest(s, _):
        slot(s)
        return 0

    lax.fori_loop(steps, last_slot + 1, rest, 0)

    for k in range(3):
        for stage in range(3):
            c_rs(stage, NG - 1, k).wait_send()
    c_d2d(NG - 1).wait_send()

    def drain(g, _):
        for k in range(3):
            c_a0(g, k).wait_send()
            c_a1(g, k).wait_send()
            c_a2(g, k).wait_send()
            c_a3(g, k, 0).wait()
            c_a3(g, k, 1).wait()
        return 0

    lax.fori_loop(0, NG, drain, 0)


def backward(x, dy, gate, up, w_gate, w_up, w_down, *, cb=256):
    rows, wide = x.shape
    ff = gate.shape[1]
    gr, half = rows // NG, wide // 2
    any_space = pl.BlockSpec(memory_space=pl.ANY)
    dma = pltpu.SemaphoreType.DMA
    grads = pl.pallas_call(
        functools.partial(kernel, cb=cb),
        out_shape=(
            pltpu.VMEM((rows, wide), BF),
            pltpu.VMEM((wide, ff), BF),
            pltpu.VMEM((wide, ff), BF),
            pltpu.VMEM((ff, wide), BF),
            jax.ShapeDtypeStruct((rows, 2 * ff), BF),
            jax.ShapeDtypeStruct((ff, rows), BF),
        ),
        in_specs=[any_space] * 7,
        out_specs=(*[pl.BlockSpec(memory_space=pltpu.VMEM)] * 4, any_space, any_space),
        scratch_shapes=[
            pltpu.VMEM((gr // 2, half), F32),
            pltpu.VMEM((gr // 4, half), F32),
            pltpu.VMEM((gr // 8, half), F32),
            pltpu.VMEM((gr, half), BF),
            pltpu.VMEM((gr // 2, half), BF),
            pltpu.VMEM((gr // 4, half), BF),
            pltpu.VMEM((gr // 8, half), BF),
            dma((10,)),
            dma(()),
            dma((NG,)),
            dma((3,)),
            dma((3,)),
            dma((3,)),
            *[dma((3, NG))] * 3,
            *[dma((3, NG))] * 6,
            *[dma((2, 3, NG))] * 2,
            pltpu.SemaphoreType.REGULAR,
        ],
        compiler_params=pltpu.CompilerParams(
            collective_id=0, has_side_effects=True, vmem_limit_bytes=22_400_000
        ),
        name="mlp_backward",
    )(x, dy, gate, up, w_gate, w_up, w_down)
    return grads[:4]


def solution(mesh):
    tokens, columns, rows = P("dp", None), P(None, "tp"), P("tp", None)
    return jax.shard_map(
        backward,
        mesh=mesh,
        in_specs=(tokens, tokens, P("dp", "tp"), P("dp", "tp"), columns, columns, rows),
        out_specs=(tokens, P("dp", "tp"), P("dp", "tp"), P(("dp", "tp"), None)),
        check_vma=False,
    )
```

```python
import functools

import jax
import jax.numpy as jnp
from jax import lax
from jax.experimental import pallas as pl
from jax.experimental.pallas import tpu as pltpu
from jax.sharding import PartitionSpec as P

MESH = pl.DeviceIdType.MESH
BF, F32 = jnp.bfloat16, jnp.float32
NT = (((1,), (1,)), ((), ()))
TN = (((0,), (0,)), ((), ()))
NN = (((1,), (0,)), ((), ()))
NG = 8
ORDERS = ((8, 4, 2), (4, 2, 8), (2, 8, 4))


def dot(a, b, dims):
    return lax.dot_general(a, b, dims, preferred_element_type=F32)


def colours(half):
    tiles = half // 128
    widths = [128 * ((tiles + 2 - k) // 3) for k in range(3)]
    return [(sum(widths[:k]), widths[k]) for k in range(3)]


def kernel(
    x, dy, gate, up, w_gate, w_up, w_down,
    dx, dw_gate, dw_up, dw_down, d_kept, hid_kept,
    acc1, acc2, acc3, d2d_out, out1, out2, out3,
    load, d2d_s, d2d_r, s1, s2, s3, r1, r2, r3, a3s, a3r, a2s, a2r, a1s, a1r, ds, dr, credit,
    *, cb,
):
    rows, wide = x.shape
    ff = gate.shape[1]
    g_rows, half = rows // NG, wide // 2
    cols = colours(half)
    steps = wide // cb
    me = lax.axis_index("tp")
    core = lax.rem(me, 2)
    sib = me + 1 - 2 * core
    mine = pl.multiple_of(core * half, 128)
    other = pl.multiple_of((1 - core) * half, 128)

    def stride_of(k, stage):
        first, second = ORDERS[k][stage], ORDERS[(k + 1) % 3][stage]
        return first + core * (second - first)

    def bit(stride):
        return lax.rem(lax.div(me, stride), 2)

    def peer(stride):
        return me + (1 - 2 * bit(stride)) * stride

    def rows_at(start, size):
        return pl.ds(pl.multiple_of(start, size), size)

    def remote(src, dst, send, recv, to):
        return pltpu.make_async_remote_copy(
            src_ref=src, dst_ref=dst, send_sem=send, recv_sem=recv,
            device_id={"tp": to}, device_id_type=MESH,
        )

    def own(g, k, start, size):
        return rows_at(start + g * g_rows, size), pl.ds(pl.multiple_of(mine + cols[k][0], 128), cols[k][1])

    def landing(g, k, stage, b):
        h = g_rows // 2
        start, size = ((b * h, h), ((1 - b) * h, h // 2), ((1 - b) * h + h // 2, h // 4))[stage]
        return start, size

    def came(g, k, stage, start, size):
        first, _ = landing(g, k, stage, bit(stride_of(k, 0)))
        return dx[own(g, k, first + start, size)].astype(F32)

    def c_d2d(g):
        return remote(d2d_out, dx.at[rows_at(g * g_rows, g_rows), pl.ds(mine, half)], d2d_s, d2d_r.at[lax.rem(g, 2)], sib)

    def c_rs(stage, g, k):
        src, send, recv = ((out1, s1, r1), (out2, s2, r2), (out3, s3, r3))[stage]
        b = bit(stride_of(k, 0))
        dst = own(g, k, *landing(g, k, stage, 1 - b if stage == 0 else b))
        return remote(src.at[:, pl.ds(*cols[k])], dx.at[dst], send.at[k], recv.at[k, lax.rem(g, 2)], peer(stride_of(k, stage)))

    def held(k, depth):
        start, size = 0, g_rows
        for stage in range(depth):
            size //= 2
            start = start + bit(stride_of(k, stage)) * size
        return start, size

    def region(g, k, depth):
        return dx.at[own(g, k, *held(k, depth))]

    def c_a0(g, k):
        return remote(region(g, k, 3), region(g, k, 3), a3s.at[k], a3r.at[k, g], peer(stride_of(k, 2)))

    def c_a1(g, k):
        return remote(region(g, k, 2), region(g, k, 2), a2s.at[k], a2r.at[k, g], peer(stride_of(k, 1)))

    def c_a2(g, k):
        return remote(region(g, k, 1), region(g, k, 1), a1s.at[k], a1r.at[k, g], peer(stride_of(k, 0)))

    def c_a3(g, k, late):
        start, size = held(k, 1)
        rows_to = dx.at[own(g, k, size - start if late else start, size)]
        return remote(rows_to, rows_to, ds.at[k], dr.at[k], sib)

    def e1(g, acc0):
        c_d2d(g).wait_recv()
        h = g_rows // 2

        def chip_sum(k, start):
            theirs = dx[rows_at(g * g_rows + start, h), pl.ds(pl.multiple_of(other + cols[k][0], 128), cols[k][1])]
            return acc0[rows_at(start, h), pl.ds(*cols[k])] + theirs.astype(F32)

        for k in range(3):

            @pl.when(g > 0)
            def _():
                c_rs(0, g, k).wait_send()

            out1[:, pl.ds(*cols[k])] = chip_sum(k, (1 - bit(stride_of(k, 0))) * h).astype(BF)
            c_rs(0, g, k).start()
        for k in range(3):
            acc1[:, pl.ds(*cols[k])] = chip_sum(k, bit(stride_of(k, 0)) * h)

    def e_mid(stage, g, src, out, dst):
        h = src.shape[0] // 2
        for k in range(3):
            c = pl.ds(*cols[k])
            c_rs(stage - 1, g, k).wait_recv()
            away = (1 - bit(stride_of(k, stage))) * h
            keep = bit(stride_of(k, stage)) * h

            @pl.when(g > 0)
            def _():
                c_rs(stage, g, k).wait_send()

            out[:, c] = (src[rows_at(away, h), c] + came(g, k, stage - 1, away, h)).astype(BF)
            c_rs(stage, g, k).start()
            dst[:, c] = src[rows_at(keep, h), c] + came(g, k, stage - 1, keep, h)

    def e4(g):
        for k in range(3):
            c_rs(2, g, k).wait_recv()
            size = acc3.shape[0]
            total = acc3[:, pl.ds(*cols[k])] + came(g, k, 2, 0, size)
            dx[own(g, k, *held(k, 3))] = total.astype(BF)

    def a0(g):
        for k in range(3):
            c_a0(g, k).start()

    def at(cond, f, g):
        @pl.when(cond)
        def _():
            f(g)

    def reduce_events(t):
        at((t >= 3) & (t < NG + 3), e4, t - 3)
        at((t >= 2) & (t < NG + 2), lambda g: e_mid(2, g, acc2, out3, acc3), t - 2)
        at((t >= 1) & (t < NG + 1), lambda g: e_mid(1, g, acc1, out2, acc2), t - 1)

    def a1(g):
        for k in range(3):
            c_a0(g, k).wait_recv()
            c_a1(g, k).start()

    def a2(g):
        for k in range(3):
            c_a1(g, k).wait_recv()
            c_a2(g, k).start()
        for k in range(3):
            c_a3(g, k, 0).start()

    def a3(g):
        for k in range(3):
            c_a2(g, k).wait_recv()
            c_a3(g, k, 1).start()

    def slot(s):
        @pl.when(s < 3)
        def _():
            reduce_events(NG + s)
            at(s >= 0, a0, NG + s - 3)

        @pl.when(s == 2)
        def _():
            for to in (sib, peer(8), peer(4), peer(2)):
                pl.semaphore_signal(credit, inc=1, device_id={"tp": to}, device_id_type=MESH)

        @pl.when(s == 3)
        def _():
            pl.semaphore_wait(credit, 4)

        for first, num, den, f in ((7, 9, 5, a3), (3, 3, 2, a2), (1, 1, 1, a1)):
            t = den * jnp.maximum(s - first, 0)
            g = lax.div(t, num)
            at((s >= first) & (lax.rem(t, num) < den) & (g < NG), f, g)

    last_slot = 7 + (9 * (NG - 1) + 4) // 5

    barrier = pltpu.get_barrier_semaphore()
    for to in (sib, peer(8), peer(4), peer(2)):
        pl.semaphore_signal(barrier, inc=1, device_id={"tp": to}, device_id_type=MESH)

    wd, wg, wu = dw_down, dw_gate, dw_up

    def first_phase(acc0, dyb, gb, ub, d_in, hid):
        def rows_of(g):
            r = rows_at(g * g_rows, g_rows)
            return (
                pltpu.make_async_copy(dy.at[r], dyb, load.at[0]),
                pltpu.make_async_copy(gate.at[r], gb, load.at[1]),
                pltpu.make_async_copy(up.at[r], ub, load.at[2]),
            )

        def keep(g):
            r = rows_at(g * g_rows, g_rows)
            return (
                pltpu.make_async_copy(d_in, d_kept.at[r], load.at[8]),
                pltpu.make_async_copy(hid, hid_kept.at[:, r], load.at[9]),
            )

        def w_half(start, i):
            r = pl.ds(start, half)
            return [
                pltpu.make_async_copy(w.at[r], v.at[r], load.at[4 + 2 * i + j])
                for j, (w, v) in enumerate(((w_gate, wg), (w_up, wu)))
            ]

        w_first = pltpu.make_async_copy(w_down, wd, load.at[3])
        w_other, w_mine = w_half(other, 0), w_half(mine, 1)
        for c in (w_first, *rows_of(0), *w_other, *w_mine):
            c.start()
        pl.semaphore_wait(barrier, 4)
        w_first.wait()

        def body(g, _):
            for c in rows_of(g):
                c.wait()

            @pl.when(g > 0)
            def _():
                for c in keep(g):
                    c.wait()
            @pl.when(g < NG)
            def _():
                acc0[:, pl.ds(0, ff)] = dot(dyb[...], wd[...], NT)

            d_h = acc0[:, pl.ds(0, ff)]
            gf, uf = gb[...].astype(F32), ub[...].astype(F32)
            sig = jax.nn.sigmoid(gf)
            silu = gf * sig

            d_in[:, pl.ds(0, ff)] = (d_h * uf * (sig + silu * (1 - sig))).astype(BF)
            d_in[:, pl.ds(ff, ff)] = (d_h * silu).astype(BF)
            hid[...] = (silu * uf).astype(BF).T
            for c in keep(g):
                c.start()

            @pl.when(g < NG - 1)
            def _():
                for c in rows_of(jnp.minimum(g + 1, NG - 1)):
                    c.start()

            def when_first(copies):
                @pl.when(g == 0)
                def _():
                    for c in copies:
                        c.wait()

            def term(start):
                w = pl.ds(start, half)
                return dot(d_in[:, pl.ds(0, ff)], wg[w, :], NT) + dot(d_in[:, pl.ds(ff, ff)], wu[w, :], NT)

            when_first(w_other)

            @pl.when(g > 0)
            def _():
                c_d2d(g).wait_send()

            @pl.when(g < NG)
            def _():
                acc0[...] = term(other)

            d2d_out[...] = acc0[...].astype(BF)

            c_d2d(g).start()
            reduce_events(g)
            when_first(w_mine)
            @pl.when(g < NG)
            def _():
                acc0[...] = term(mine)

            e1(g, acc0)
            return 0

        lax.fori_loop(0, NG, body, 0)
        for c in keep(NG - 1):
            c.wait()

    pl.run_scoped(
        first_phase,
        pltpu.VMEM((g_rows, half), F32),
        pltpu.VMEM((g_rows, wide), BF),
        pltpu.VMEM((g_rows, ff), BF),
        pltpu.VMEM((g_rows, ff), BF),
        pltpu.VMEM((g_rows, 2 * ff), BF),
        pltpu.VMEM((ff, g_rows), BF),
    )

    def second_phase(d_all, hid_t, xb, yb):
        again = (pltpu.make_async_copy(d_kept, d_all, load.at[8]), pltpu.make_async_copy(hid_kept, hid_t, load.at[9]))
        for c in again:
            c.start()

        def loads(i, b):
            c = rows_at(i * cb, cb)
            return (
                pltpu.make_async_copy(x.at[:, c], xb.at[b], load.at[b]),
                pltpu.make_async_copy(dy.at[:, c], yb.at[b], load.at[2 + b]),
            )

        for c in loads(0, 0):
            c.start()

        def early(g, _):
            a0(g)
            return 0

        lax.fori_loop(0, NG - 3, early, 0)
        for c in again:
            c.wait()

        def body(i, _):
            b = lax.rem(i, 2)

            @pl.when(i < steps - 1)
            def _():
                for c in loads(jnp.minimum(i + 1, steps - 1), 1 - b):
                    c.start()

            into = loads(i, b)
            c = rows_at(i * cb, cb)
            into[0].wait()

            @pl.when(i < steps)
            def _():
                both = dot(xb[b], d_all[...], TN).astype(BF)
                dw_gate[c, :] = both[:, :ff]
                dw_up[c, :] = both[:, ff:]

            into[1].wait()

            @pl.when(i < steps)
            def _():
                dw_down[:, c] = dot(hid_t[...], yb[b], NN).astype(BF)

            slot(i)
            return 0

        lax.fori_loop(0, steps, body, 0)

    pl.run_scoped(
        second_phase,
        pltpu.VMEM((rows, 2 * ff), BF),
        pltpu.VMEM((ff, rows), BF),
        pltpu.VMEM((2, rows, cb), BF),
        pltpu.VMEM((2, rows, cb), BF),
    )

    def rest(s, _):
        slot(s)
        return 0

    lax.fori_loop(steps, last_slot + 1, rest, 0)

    for k in range(3):
        for stage in range(3):
            c_rs(stage, NG - 1, k).wait_send()
    c_d2d(NG - 1).wait_send()

    for k in range(3):
        for sem, part in ((a3s, 8), (a2s, 4), (a1s, 2), (ds, 1), (dr, 1)):
            whole = dx.at[pl.ds(0, rows // part), pl.ds(*cols[k])]
            pltpu.make_async_copy(whole, whole, sem.at[k]).wait()


def backward(x, dy, gate, up, w_gate, w_up, w_down, *, cb=256):
    rows, wide = x.shape
    ff = gate.shape[1]
    gr, half = rows // NG, wide // 2
    any_space = pl.BlockSpec(memory_space=pl.ANY)
    dma = pltpu.SemaphoreType.DMA
    grads = pl.pallas_call(
        functools.partial(kernel, cb=cb),
        out_shape=(
            pltpu.VMEM((rows, wide), BF),
            pltpu.VMEM((wide, ff), BF),
            pltpu.VMEM((wide, ff), BF),
            pltpu.VMEM((ff, wide), BF),
            jax.ShapeDtypeStruct((rows, 2 * ff), BF),
            jax.ShapeDtypeStruct((ff, rows), BF),
        ),
        in_specs=[any_space] * 7,
        out_specs=(*[pl.BlockSpec(memory_space=pltpu.VMEM)] * 4, any_space, any_space),
        scratch_shapes=[
            pltpu.VMEM((gr // 2, half), F32),
            pltpu.VMEM((gr // 4, half), F32),
            pltpu.VMEM((gr // 8, half), F32),
            pltpu.VMEM((gr, half), BF),
            pltpu.VMEM((gr // 2, half), BF),
            pltpu.VMEM((gr // 4, half), BF),
            pltpu.VMEM((gr // 8, half), BF),
            dma((10,)),
            dma(()),
            dma((2,)),
            dma((3,)),
            dma((3,)),
            dma((3,)),
            *[dma((3, 2))] * 3,
            *[dma((3,)), dma((3, NG))] * 3,
            *[dma((3,))] * 2,
            pltpu.SemaphoreType.REGULAR,
        ],
        compiler_params=pltpu.CompilerParams(
            collective_id=0, has_side_effects=True, vmem_limit_bytes=22_400_000
        ),
        name="mlp_backward",
    )(x, dy, gate, up, w_gate, w_up, w_down)
    return grads[:4]


def solution(mesh):
    tokens, columns, rows = P("dp", None), P(None, "tp"), P("tp", None)
    return jax.shard_map(
        backward,
        mesh=mesh,
        in_specs=(tokens, tokens, P("dp", "tp"), P("dp", "tp"), columns, columns, rows),
        out_specs=(tokens, P("dp", "tp"), P("dp", "tp"), P(("dp", "tp"), None)),
        check_vma=False,
    )
```

```python
import functools

import jax
import jax.numpy as jnp
from jax import lax
from jax.experimental import pallas as pl
from jax.experimental.pallas import tpu as pltpu
from jax.sharding import PartitionSpec as P

MESH = pl.DeviceIdType.MESH
BF, F32 = jnp.bfloat16, jnp.float32
NT = (((1,), (1,)), ((), ()))
TN = (((0,), (0,)), ((), ()))
NN = (((1,), (0,)), ((), ()))
NG = 8
ORDERS = ((8, 4, 2), (4, 2, 8), (2, 8, 4))
SECOND = ((2, 4, 8), (8, 2, 4), (4, 8, 2))


def dot(a, b, dims):
    return lax.dot_general(a, b, dims, preferred_element_type=F32)


def colours(half):
    tiles = half // 128
    widths = [128 * ((tiles + 2 - k) // 3) for k in range(3)]
    return [(sum(widths[:k]), widths[k]) for k in range(3)]


def kernel(
    x, dy, gate, up, w_gate, w_up, w_down,
    dx, dw_gate, dw_up, dw_down, d_kept, hid_kept,
    acc1, acc2, acc3, d2d_out, out1, out2, out3,
    load, d2d_s, d2d_r, s1, s2, s3, r1, r2, r3, a3s, a3r, a2s, a2r, a1s, a1r, ds, dr, credit,
    *, cb,
):
    rows, wide = x.shape
    ff = gate.shape[1]
    g_rows, half = rows // NG, wide // 2
    cols = colours(half)
    steps = wide // cb
    me = lax.axis_index("tp")
    core = lax.rem(me, 2)
    sib = me + 1 - 2 * core
    mine = pl.multiple_of(core * half, 128)
    other = pl.multiple_of((1 - core) * half, 128)

    def stride_of(k, stage):
        first, second = ORDERS[k][stage], SECOND[k][stage]
        return first + core * (second - first)

    def bit(stride):
        return lax.rem(lax.div(me, stride), 2)

    def peer(stride):
        return me + (1 - 2 * bit(stride)) * stride

    def rows_at(start, size):
        return pl.ds(pl.multiple_of(start, size), size)

    def remote(src, dst, send, recv, to):
        return pltpu.make_async_remote_copy(
            src_ref=src, dst_ref=dst, send_sem=send, recv_sem=recv,
            device_id={"tp": to}, device_id_type=MESH,
        )

    def own(g, k, start, size):
        return rows_at(start + g * g_rows, size), pl.ds(pl.multiple_of(mine + cols[k][0], 128), cols[k][1])

    def landing(g, k, stage, b):
        h = g_rows // 2
        start, size = ((b * h, h), ((1 - b) * h, h // 2), ((1 - b) * h + h // 2, h // 4))[stage]
        return start, size

    def came(g, k, stage, start, size):
        first, _ = landing(g, k, stage, bit(stride_of(k, 0)))
        return dx[own(g, k, first + start, size)].astype(F32)

    def c_d2d(g, k):
        dst = dx.at[own(g, k, 0, g_rows)]
        return remote(d2d_out.at[:, pl.ds(*cols[k])], dst, d2d_s.at[k], d2d_r.at[k, lax.rem(g, 2)], sib)

    def c_rs(stage, g, k):
        src, send, recv = ((out1, s1, r1), (out2, s2, r2), (out3, s3, r3))[stage]
        b = bit(stride_of(k, 0))
        dst = own(g, k, *landing(g, k, stage, 1 - b if stage == 0 else b))
        return remote(src.at[:, pl.ds(*cols[k])], dx.at[dst], send.at[k], recv.at[k, lax.rem(g, 2)], peer(stride_of(k, stage)))

    def held(k, depth):
        start, size = 0, g_rows
        for stage in range(depth):
            size //= 2
            start = start + bit(stride_of(k, stage)) * size
        return start, size

    def region(g, k, depth):
        return dx.at[own(g, k, *held(k, depth))]

    def c_a0(g, k):
        return remote(region(g, k, 3), region(g, k, 3), a3s.at[k], a3r.at[k, g], peer(stride_of(k, 2)))

    def c_a1(g, k):
        return remote(region(g, k, 2), region(g, k, 2), a2s.at[k], a2r.at[k, g], peer(stride_of(k, 1)))

    def c_a2(g, k):
        return remote(region(g, k, 1), region(g, k, 1), a1s.at[k], a1r.at[k, g], peer(stride_of(k, 0)))

    def c_a3(g, k, late):
        start, size = held(k, 1)
        rows_to = dx.at[own(g, k, size - start if late else start, size)]
        return remote(rows_to, rows_to, ds.at[k], dr.at[k], sib)

    def e1(g, acc0):
        h = g_rows // 2

        def chip_sum(k, start):
            theirs = dx[rows_at(g * g_rows + start, h), pl.ds(pl.multiple_of(other + cols[k][0], 128), cols[k][1])]
            return acc0[rows_at(start, h), pl.ds(*cols[k])] + theirs.astype(F32)

        for k in range(3):
            c_d2d(g, k).wait_recv()

            @pl.when(g > 0)
            def _():
                c_rs(0, g, k).wait_send()

            out1[:, pl.ds(*cols[k])] = chip_sum(k, (1 - bit(stride_of(k, 0))) * h).astype(BF)
            c_rs(0, g, k).start()
        for k in range(3):
            acc1[:, pl.ds(*cols[k])] = chip_sum(k, bit(stride_of(k, 0)) * h)

    def e_mid(stage, g, src, out, dst):
        h = src.shape[0] // 2
        for k in range(3):
            c = pl.ds(*cols[k])
            c_rs(stage - 1, g, k).wait_recv()
            away = (1 - bit(stride_of(k, stage))) * h
            keep = bit(stride_of(k, stage)) * h

            @pl.when(g > 0)
            def _():
                c_rs(stage, g, k).wait_send()

            out[:, c] = (src[rows_at(away, h), c] + came(g, k, stage - 1, away, h)).astype(BF)
            c_rs(stage, g, k).start()
            dst[:, c] = src[rows_at(keep, h), c] + came(g, k, stage - 1, keep, h)

    def e4(g):
        for k in range(3):
            c_rs(2, g, k).wait_recv()
            size = acc3.shape[0]
            total = acc3[:, pl.ds(*cols[k])] + came(g, k, 2, 0, size)
            dx[own(g, k, *held(k, 3))] = total.astype(BF)

    def a0(g):
        for k in range(3):
            c_a0(g, k).start()

    def early(g, _):
        a0(g)
        return 0

    def at(cond, f, g):
        @pl.when(cond)
        def _():
            f(g)

    def reduce_events(t):
        at((t >= 3) & (t < NG + 3), e4, t - 3)
        at((t >= 2) & (t < NG + 2), lambda g: e_mid(2, g, acc2, out3, acc3), t - 2)
        at((t >= 1) & (t < NG + 1), lambda g: e_mid(1, g, acc1, out2, acc2), t - 1)

    def a1(g):
        for k in range(3):
            c_a0(g, k).wait_recv()
            c_a1(g, k).start()

    def a2(g):
        for k in range(3):
            c_a1(g, k).wait_recv()
            c_a2(g, k).start()
        for k in range(3):
            c_a3(g, k, 0).start()

    def a3(g):
        for k in range(3):
            c_a2(g, k).wait_recv()
            c_a3(g, k, 1).start()

    def slot(s):
        @pl.when(s < 3)
        def _():
            reduce_events(NG + s)
            at(s >= 0, a0, NG + s - 3)

            @pl.when(s == 0)
            def _():
                lax.fori_loop(2, NG - 3, early, 0)

        @pl.when(s == 2)
        def _():
            for to in (sib, peer(8), peer(4), peer(2)):
                pl.semaphore_signal(credit, inc=1, device_id={"tp": to}, device_id_type=MESH)

        @pl.when(s == 3)
        def _():
            pl.semaphore_wait(credit, 4)

        for first, num, den, f in ((9, 8, 5, a3), (3, 3, 2, a2), (1, 1, 1, a1)):
            t = den * jnp.maximum(s - first, 0)
            g = lax.div(t, num)
            at((s >= first) & (lax.rem(t, num) < den) & (g < NG), f, g)

    last_slot = 9 + (8 * (NG - 1) + 4) // 5

    barrier = pltpu.get_barrier_semaphore()
    for to in (sib, peer(8), peer(4), peer(2)):
        pl.semaphore_signal(barrier, inc=1, device_id={"tp": to}, device_id_type=MESH)

    wd, wg, wu = dw_down, dw_gate, dw_up

    def first_phase(acc0, dyb, gb, ub, d_in, hid):
        def rows_of(g):
            r = rows_at(g * g_rows, g_rows)
            return (
                pltpu.make_async_copy(dy.at[r], dyb, load.at[0]),
                pltpu.make_async_copy(gate.at[r], gb, load.at[1]),
                pltpu.make_async_copy(up.at[r], ub, load.at[2]),
            )

        def keep(g):
            r = rows_at(g * g_rows, g_rows)
            return (
                pltpu.make_async_copy(d_in, d_kept.at[r], load.at[8]),
                pltpu.make_async_copy(hid, hid_kept.at[:, r], load.at[9]),
            )

        def w_half(start, i):
            r = pl.ds(start, half)
            return [
                pltpu.make_async_copy(w.at[r], v.at[r], load.at[4 + 2 * i + j])
                for j, (w, v) in enumerate(((w_gate, wg), (w_up, wu)))
            ]

        w_first = pltpu.make_async_copy(w_down, wd, load.at[3])
        w_other, w_mine = w_half(other, 0), w_half(mine, 1)
        for c in (w_first, *rows_of(0), *w_other, *w_mine):
            c.start()
        pl.semaphore_wait(barrier, 4)
        w_first.wait()

        def body(g, _):
            for c in rows_of(g):
                c.wait()

            @pl.when(g > 0)
            def _():
                for c in keep(g):
                    c.wait()
            @pl.when(g < NG)
            def _():
                acc0[:, pl.ds(0, ff)] = dot(dyb[...], wd[...], NT)

            d_h = acc0[:, pl.ds(0, ff)]
            gf, uf = gb[...].astype(F32), ub[...].astype(F32)
            sig = jax.nn.sigmoid(gf)
            silu = gf * sig

            d_in[:, pl.ds(0, ff)] = (d_h * uf * (sig + silu * (1 - sig))).astype(BF)
            d_in[:, pl.ds(ff, ff)] = (d_h * silu).astype(BF)
            hid[...] = (silu * uf).astype(BF).T
            for c in keep(g):
                c.start()

            @pl.when(g < NG - 1)
            def _():
                for c in rows_of(jnp.minimum(g + 1, NG - 1)):
                    c.start()

            def when_first(copies):
                @pl.when(g == 0)
                def _():
                    for c in copies:
                        c.wait()

            def term(start):
                w = pl.ds(start, half)
                return dot(d_in[:, pl.ds(0, ff)], wg[w, :], NT) + dot(d_in[:, pl.ds(ff, ff)], wu[w, :], NT)

            when_first(w_other)

            @pl.when(g > 0)
            def _():
                for k in range(3):
                    c_d2d(g, k).wait_send()

            @pl.when(g < NG)
            def _():
                acc0[...] = term(other)

            d2d_out[...] = acc0[...].astype(BF)

            for k in range(3):
                c_d2d(g, k).start()
            reduce_events(g)
            when_first(w_mine)
            @pl.when(g < NG)
            def _():
                acc0[...] = term(mine)

            e1(g, acc0)
            return 0

        lax.fori_loop(0, NG, body, 0)
        for c in keep(NG - 1):
            c.wait()

    pl.run_scoped(
        first_phase,
        pltpu.VMEM((g_rows, half), F32),
        pltpu.VMEM((g_rows, wide), BF),
        pltpu.VMEM((g_rows, ff), BF),
        pltpu.VMEM((g_rows, ff), BF),
        pltpu.VMEM((g_rows, 2 * ff), BF),
        pltpu.VMEM((ff, g_rows), BF),
    )

    def second_phase(d_all, hid_t, xb, yb):
        again = (pltpu.make_async_copy(d_kept, d_all, load.at[8]), pltpu.make_async_copy(hid_kept, hid_t, load.at[9]))
        for c in again:
            c.start()

        def loads(i, b):
            c = rows_at(i * cb, cb)
            return (
                pltpu.make_async_copy(x.at[:, c], xb.at[b], load.at[b]),
                pltpu.make_async_copy(dy.at[:, c], yb.at[b], load.at[2 + b]),
            )

        for c in loads(0, 0):
            c.start()

        lax.fori_loop(0, 2, early, 0)
        for c in again:
            c.wait()

        def body(i, _):
            b = lax.rem(i, 2)

            @pl.when(i < steps - 1)
            def _():
                for c in loads(jnp.minimum(i + 1, steps - 1), 1 - b):
                    c.start()

            into = loads(i, b)
            c = rows_at(i * cb, cb)
            into[0].wait()

            @pl.when(i < steps)
            def _():
                both = dot(xb[b], d_all[...], TN).astype(BF)
                dw_gate[c, :] = both[:, :ff]
                dw_up[c, :] = both[:, ff:]

            into[1].wait()

            @pl.when(i < steps)
            def _():
                dw_down[:, c] = dot(hid_t[...], yb[b], NN).astype(BF)

            slot(i)
            return 0

        lax.fori_loop(0, steps, body, 0)

    pl.run_scoped(
        second_phase,
        pltpu.VMEM((rows, 2 * ff), BF),
        pltpu.VMEM((ff, rows), BF),
        pltpu.VMEM((2, rows, cb), BF),
        pltpu.VMEM((2, rows, cb), BF),
    )

    def rest(s, _):
        slot(s)
        return 0

    lax.fori_loop(steps, last_slot + 1, rest, 0)

    for k in range(3):
        for stage in range(3):
            c_rs(stage, NG - 1, k).wait_send()
        c_d2d(NG - 1, k).wait_send()

    for k in range(3):
        for sem, part in ((a3s, 8), (a2s, 4), (a1s, 2), (ds, 1), (dr, 1)):
            whole = dx.at[pl.ds(0, rows // part), pl.ds(*cols[k])]
            pltpu.make_async_copy(whole, whole, sem.at[k]).wait()


def backward(x, dy, gate, up, w_gate, w_up, w_down, *, cb=256):
    rows, wide = x.shape
    ff = gate.shape[1]
    gr, half = rows // NG, wide // 2
    any_space = pl.BlockSpec(memory_space=pl.ANY)
    dma = pltpu.SemaphoreType.DMA
    grads = pl.pallas_call(
        functools.partial(kernel, cb=cb),
        out_shape=(
            pltpu.VMEM((rows, wide), BF),
            pltpu.VMEM((wide, ff), BF),
            pltpu.VMEM((wide, ff), BF),
            pltpu.VMEM((ff, wide), BF),
            jax.ShapeDtypeStruct((rows, 2 * ff), BF),
            jax.ShapeDtypeStruct((ff, rows), BF),
        ),
        in_specs=[any_space] * 7,
        out_specs=(*[pl.BlockSpec(memory_space=pltpu.VMEM)] * 4, any_space, any_space),
        scratch_shapes=[
            pltpu.VMEM((gr // 2, half), F32),
            pltpu.VMEM((gr // 4, half), F32),
            pltpu.VMEM((gr // 8, half), F32),
            pltpu.VMEM((gr, half), BF),
            pltpu.VMEM((gr // 2, half), BF),
            pltpu.VMEM((gr // 4, half), BF),
            pltpu.VMEM((gr // 8, half), BF),
            dma((10,)),
            dma((3,)),
            dma((3, 2)),
            dma((3,)),
            dma((3,)),
            dma((3,)),
            *[dma((3, 2))] * 3,
            *[dma((3,)), dma((3, NG))] * 3,
            *[dma((3,))] * 2,
            pltpu.SemaphoreType.REGULAR,
        ],
        compiler_params=pltpu.CompilerParams(
            collective_id=0, has_side_effects=True, vmem_limit_bytes=22_400_000
        ),
        name="mlp_backward",
    )(x, dy, gate, up, w_gate, w_up, w_down)
    return grads[:4]


def solution(mesh):
    tokens, columns, rows = P("dp", None), P(None, "tp"), P("tp", None)
    return jax.shard_map(
        backward,
        mesh=mesh,
        in_specs=(tokens, tokens, P("dp", "tp"), P("dp", "tp"), columns, columns, rows),
        out_specs=(tokens, P("dp", "tp"), P("dp", "tp"), P(("dp", "tp"), None)),
        check_vma=False,
    )
```

```python
import functools

import jax
import jax.numpy as jnp
from jax import lax
from jax.experimental import pallas as pl
from jax.experimental.pallas import tpu as pltpu
from jax.sharding import PartitionSpec as P

MESH = pl.DeviceIdType.MESH
BF, F32 = jnp.bfloat16, jnp.float32
NT = (((1,), (1,)), ((), ()))
TN = (((0,), (0,)), ((), ()))
NN = (((1,), (0,)), ((), ()))
NG = 8
ORDERS = ((8, 4, 2), (4, 2, 8), (2, 8, 4))
SECOND = ((2, 4, 8), (8, 2, 4), (4, 8, 2))


def dot(a, b, dims):
    return lax.dot_general(a, b, dims, preferred_element_type=F32)


def colours(half):
    tiles = half // 128
    widths = [128 * ((tiles + 2 - k) // 3) for k in range(3)]
    return [(sum(widths[:k]), widths[k]) for k in range(3)]


def kernel(
    x, dy, gate, up, w_gate, w_up, w_down,
    dx, dw_gate, dw_up, dw_down, d_kept, hid_kept,
    acc1, acc2, acc3, d2d_out, out1, out2, out3,
    load, d2d_s, d2d_r, s1, s2, s3, r1, r2, r3, a3s, a3r, a2s, a2r, a1s, a1r, ds, dr, credit,
    *, cb,
):
    rows, wide = x.shape
    ff = gate.shape[1]
    g_rows, half = rows // NG, wide // 2
    cols = colours(half)
    steps = wide // cb
    me = lax.axis_index("tp")
    core = lax.rem(me, 2)
    sib = me + 1 - 2 * core
    mine = pl.multiple_of(core * half, 128)
    other = pl.multiple_of((1 - core) * half, 128)

    def stride_of(k, stage):
        first, second = ORDERS[k][stage], SECOND[k][stage]
        return first + core * (second - first)

    def bit(stride):
        return lax.rem(lax.div(me, stride), 2)

    def peer(stride):
        return me + (1 - 2 * bit(stride)) * stride

    def rows_at(start, size):
        return pl.ds(pl.multiple_of(start, size), size)

    def remote(src, dst, send, recv, to):
        return pltpu.make_async_remote_copy(
            src_ref=src, dst_ref=dst, send_sem=send, recv_sem=recv,
            device_id={"tp": to}, device_id_type=MESH,
        )

    def own(g, k, start, size):
        return rows_at(start + g * g_rows, size), pl.ds(pl.multiple_of(mine + cols[k][0], 128), cols[k][1])

    def landing(g, k, stage, b):
        h = g_rows // 2
        start, size = ((b * h, h), ((1 - b) * h, h // 2), ((1 - b) * h + h // 2, h // 4))[stage]
        return start, size

    def came(g, k, stage, start, size):
        first, _ = landing(g, k, stage, bit(stride_of(k, 0)))
        return dx[own(g, k, first + start, size)].astype(F32)

    def c_d2d(g, k):
        dst = dx.at[own(g, k, 0, g_rows)]
        return remote(d2d_out.at[:, pl.ds(*cols[k])], dst, d2d_s.at[k], d2d_r.at[k, lax.rem(g, 2)], sib)

    def c_rs(stage, g, k):
        src, send, recv = ((out1, s1, r1), (out2, s2, r2), (out3, s3, r3))[stage]
        b = bit(stride_of(k, 0))
        dst = own(g, k, *landing(g, k, stage, 1 - b if stage == 0 else b))
        return remote(src.at[:, pl.ds(*cols[k])], dx.at[dst], send.at[k], recv.at[k, lax.rem(g, 2)], peer(stride_of(k, stage)))

    def held(k, depth):
        start, size = 0, g_rows
        for stage in range(depth):
            size //= 2
            start = start + bit(stride_of(k, stage)) * size
        return start, size

    def region(g, k, depth):
        return dx.at[own(g, k, *held(k, depth))]

    def c_a0(g, k):
        return remote(region(g, k, 3), region(g, k, 3), a3s.at[k], a3r.at[k, g], peer(stride_of(k, 2)))

    def c_a1(g, k):
        return remote(region(g, k, 2), region(g, k, 2), a2s.at[k], a2r.at[k, g], peer(stride_of(k, 1)))

    def c_a2(g, k):
        return remote(region(g, k, 1), region(g, k, 1), a1s.at[k], a1r.at[k, g], peer(stride_of(k, 0)))

    def c_a3(g, k, late):
        start, size = held(k, 1)
        rows_to = dx.at[own(g, k, size - start if late else start, size)]
        return remote(rows_to, rows_to, ds.at[k], dr.at[k], sib)

    def e1(g, acc0):
        h = g_rows // 2

        def chip_sum(k, start):
            theirs = dx[rows_at(g * g_rows + start, h), pl.ds(pl.multiple_of(other + cols[k][0], 128), cols[k][1])]
            return acc0[rows_at(start, h), pl.ds(*cols[k])] + theirs.astype(F32)

        for k in range(3):
            c_d2d(g, k).wait_recv()

            @pl.when(g > 0)
            def _():
                c_rs(0, g, k).wait_send()

            out1[:, pl.ds(*cols[k])] = chip_sum(k, (1 - bit(stride_of(k, 0))) * h).astype(BF)
            c_rs(0, g, k).start()
        for k in range(3):
            acc1[:, pl.ds(*cols[k])] = chip_sum(k, bit(stride_of(k, 0)) * h)

    def e_mid(stage, g, src, out, dst):
        h = src.shape[0] // 2
        for k in range(3):
            c = pl.ds(*cols[k])
            c_rs(stage - 1, g, k).wait_recv()
            away = (1 - bit(stride_of(k, stage))) * h
            keep = bit(stride_of(k, stage)) * h

            @pl.when(g > 0)
            def _():
                c_rs(stage, g, k).wait_send()

            out[:, c] = (src[rows_at(away, h), c] + came(g, k, stage - 1, away, h)).astype(BF)
            c_rs(stage, g, k).start()
            dst[:, c] = src[rows_at(keep, h), c] + came(g, k, stage - 1, keep, h)

    def e4(g):
        for k in range(3):
            c_rs(2, g, k).wait_recv()
            size = acc3.shape[0]
            total = acc3[:, pl.ds(*cols[k])] + came(g, k, 2, 0, size)
            dx[own(g, k, *held(k, 3))] = total.astype(BF)

    def a0(g):
        for k in range(3):
            c_a0(g, k).start()

    def early(g, _):
        a0(g)
        return 0

    def at(cond, f, g):
        @pl.when(cond)
        def _():
            f(g)

    def reduce_events(t):
        at((t >= 3) & (t < NG + 3), e4, t - 3)
        at((t >= 2) & (t < NG + 2), lambda g: e_mid(2, g, acc2, out3, acc3), t - 2)
        at((t >= 1) & (t < NG + 1), lambda g: e_mid(1, g, acc1, out2, acc2), t - 1)

    def a1(g):
        for k in range(3):
            c_a0(g, k).wait_recv()
            c_a1(g, k).start()

    def a2(g):
        for k in range(3):
            c_a1(g, k).wait_recv()
            c_a2(g, k).start()
        for k in range(3):
            c_a3(g, k, 0).start()

    def a3(g):
        for k in range(3):
            c_a2(g, k).wait_recv()
            c_a3(g, k, 1).start()

    def slot(s):
        @pl.when(s < 3)
        def _():
            reduce_events(NG + s)
            at(s >= 0, a0, NG + s - 3)

            @pl.when(s == 0)
            def _():
                lax.fori_loop(2, NG - 3, early, 0)

        @pl.when(s == 2)
        def _():
            for to in (sib, peer(8), peer(4), peer(2)):
                pl.semaphore_signal(credit, inc=1, device_id={"tp": to}, device_id_type=MESH)

        @pl.when(s == 3)
        def _():
            pl.semaphore_wait(credit, 4)

        for first, num, den, f in ((9, 8, 5, a3), (3, 3, 2, a2), (1, 1, 1, a1)):
            t = den * jnp.maximum(s - first, 0)
            g = lax.div(t, num)
            at((s >= first) & (lax.rem(t, num) < den) & (g < NG), f, g)

    last_slot = 9 + (8 * (NG - 1) + 4) // 5

    barrier = pltpu.get_barrier_semaphore()
    for to in (sib, peer(8), peer(4), peer(2)):
        pl.semaphore_signal(barrier, inc=1, device_id={"tp": to}, device_id_type=MESH)

    wd, wg, wu = dw_down, dw_gate, dw_up

    def first_phase(acc0, dyb, gb, ub, d_in, hid):
        def rows_of(g):
            r = rows_at(g * g_rows, g_rows)
            return (
                pltpu.make_async_copy(dy.at[r], dyb, load.at[0]),
                pltpu.make_async_copy(gate.at[r], gb, load.at[1]),
                pltpu.make_async_copy(up.at[r], ub, load.at[2]),
            )

        def keep(g):
            r = rows_at(g * g_rows, g_rows)
            return (
                pltpu.make_async_copy(d_in, d_kept.at[r], load.at[8]),
                pltpu.make_async_copy(hid, hid_kept.at[:, r], load.at[9]),
            )

        def w_half(start, i):
            r = pl.ds(start, half)
            return [
                pltpu.make_async_copy(w.at[r], v.at[r], load.at[4 + 2 * i + j])
                for j, (w, v) in enumerate(((w_gate, wg), (w_up, wu)))
            ]

        w_first = pltpu.make_async_copy(w_down, wd, load.at[3])
        w_other, w_mine = w_half(other, 0), w_half(mine, 1)
        for c in (w_first, *rows_of(0), *w_other, *w_mine):
            c.start()
        pl.semaphore_wait(barrier, 4)
        w_first.wait()

        def body(g, _):
            for c in rows_of(g):
                c.wait()

            @pl.when(g > 0)
            def _():
                for c in keep(g):
                    c.wait()
            @pl.when(g < NG)
            def _():
                acc0[:, pl.ds(0, ff)] = dot(dyb[...], wd[...], NT)

            d_h = acc0[:, pl.ds(0, ff)]
            gf, uf = gb[...].astype(F32), ub[...].astype(F32)
            sig = jax.nn.sigmoid(gf)
            silu = gf * sig

            d_in[:, pl.ds(0, ff)] = (d_h * uf * (sig + silu * (1 - sig))).astype(BF)
            d_in[:, pl.ds(ff, ff)] = (d_h * silu).astype(BF)
            hid[...] = (silu * uf).astype(BF).T
            for c in keep(g):
                c.start()

            @pl.when(g < NG - 1)
            def _():
                for c in rows_of(jnp.minimum(g + 1, NG - 1)):
                    c.start()

            def when_first(copies):
                @pl.when(g == 0)
                def _():
                    for c in copies:
                        c.wait()

            def term(start):
                w = pl.ds(start, half)
                return dot(d_in[:, pl.ds(0, ff)], wg[w, :], NT) + dot(d_in[:, pl.ds(ff, ff)], wu[w, :], NT)

            when_first(w_other)

            @pl.when(g > 0)
            def _():
                for k in range(3):
                    c_d2d(g, k).wait_send()

            @pl.when(g < NG)
            def _():
                acc0[...] = term(other)

            d2d_out[...] = acc0[...].astype(BF)

            for k in range(3):
                c_d2d(g, k).start()
            reduce_events(g)
            when_first(w_mine)
            @pl.when(g < NG)
            def _():
                acc0[...] = term(mine)

            e1(g, acc0)
            return 0

        lax.fori_loop(0, NG, body, 0)
        for c in keep(NG - 1):
            c.wait()

    pl.run_scoped(
        first_phase,
        pltpu.VMEM((g_rows, half), F32),
        pltpu.VMEM((g_rows, wide), BF),
        pltpu.VMEM((g_rows, ff), BF),
        pltpu.VMEM((g_rows, ff), BF),
        pltpu.VMEM((g_rows, 2 * ff), BF),
        pltpu.VMEM((ff, g_rows), BF),
    )

    def second_phase(d_all, hid_t, xb, yb):
        again = (pltpu.make_async_copy(d_kept, d_all, load.at[8]), pltpu.make_async_copy(hid_kept, hid_t, load.at[9]))
        def loads(i, b):
            c = rows_at(i * cb, cb)
            return (
                pltpu.make_async_copy(x.at[:, c], xb.at[b], load.at[b]),
                pltpu.make_async_copy(dy.at[:, c], yb.at[b], load.at[2 + b]),
            )

        first = loads(0, 0)
        for c in (first[0], again[0], first[1], again[1]):
            c.start()

        lax.fori_loop(0, 2, early, 0)
        again[0].wait()

        def body(i, _):
            b = lax.rem(i, 2)

            @pl.when(i < steps - 1)
            def _():
                for c in loads(jnp.minimum(i + 1, steps - 1), 1 - b):
                    c.start()

            into = loads(i, b)
            c = rows_at(i * cb, cb)
            into[0].wait()

            @pl.when(i < steps)
            def _():
                both = dot(xb[b], d_all[...], TN).astype(BF)
                dw_gate[c, :] = both[:, :ff]
                dw_up[c, :] = both[:, ff:]

            into[1].wait()

            @pl.when(i == 0)
            def _():
                again[1].wait()

            @pl.when(i < steps)
            def _():
                dw_down[:, c] = dot(hid_t[...], yb[b], NN).astype(BF)

            slot(i)
            return 0

        lax.fori_loop(0, steps, body, 0)

    pl.run_scoped(
        second_phase,
        pltpu.VMEM((rows, 2 * ff), BF),
        pltpu.VMEM((ff, rows), BF),
        pltpu.VMEM((2, rows, cb), BF),
        pltpu.VMEM((2, rows, cb), BF),
    )

    def rest(s, _):
        slot(s)
        return 0

    lax.fori_loop(steps, last_slot + 1, rest, 0)

    for k in range(3):
        for stage in range(3):
            c_rs(stage, NG - 1, k).wait_send()
        c_d2d(NG - 1, k).wait_send()

    for k in range(3):
        for sem, part in ((a3s, 8), (a2s, 4), (a1s, 2), (ds, 1), (dr, 1)):
            whole = dx.at[pl.ds(0, rows // part), pl.ds(*cols[k])]
            pltpu.make_async_copy(whole, whole, sem.at[k]).wait()


def backward(x, dy, gate, up, w_gate, w_up, w_down, *, cb=256):
    rows, wide = x.shape
    ff = gate.shape[1]
    gr, half = rows // NG, wide // 2
    any_space = pl.BlockSpec(memory_space=pl.ANY)
    dma = pltpu.SemaphoreType.DMA
    grads = pl.pallas_call(
        functools.partial(kernel, cb=cb),
        out_shape=(
            pltpu.VMEM((rows, wide), BF),
            pltpu.VMEM((wide, ff), BF),
            pltpu.VMEM((wide, ff), BF),
            pltpu.VMEM((ff, wide), BF),
            jax.ShapeDtypeStruct((rows, 2 * ff), BF),
            jax.ShapeDtypeStruct((ff, rows), BF),
        ),
        in_specs=[any_space] * 7,
        out_specs=(*[pl.BlockSpec(memory_space=pltpu.VMEM)] * 4, any_space, any_space),
        scratch_shapes=[
            pltpu.VMEM((gr // 2, half), F32),
            pltpu.VMEM((gr // 4, half), F32),
            pltpu.VMEM((gr // 8, half), F32),
            pltpu.VMEM((gr, half), BF),
            pltpu.VMEM((gr // 2, half), BF),
            pltpu.VMEM((gr // 4, half), BF),
            pltpu.VMEM((gr // 8, half), BF),
            dma((10,)),
            dma((3,)),
            dma((3, 2)),
            dma((3,)),
            dma((3,)),
            dma((3,)),
            *[dma((3, 2))] * 3,
            *[dma((3,)), dma((3, NG))] * 3,
            *[dma((3,))] * 2,
            pltpu.SemaphoreType.REGULAR,
        ],
        compiler_params=pltpu.CompilerParams(
            collective_id=0, has_side_effects=True, vmem_limit_bytes=22_400_000
        ),
        name="mlp_backward",
    )(x, dy, gate, up, w_gate, w_up, w_down)
    return grads[:4]


def solution(mesh):
    tokens, columns, rows = P("dp", None), P(None, "tp"), P("tp", None)
    return jax.shard_map(
        backward,
        mesh=mesh,
        in_specs=(tokens, tokens, P("dp", "tp"), P("dp", "tp"), columns, columns, rows),
        out_specs=(tokens, P("dp", "tp"), P("dp", "tp"), P(("dp", "tp"), None)),
        check_vma=False,
    )
```
